16 devices in a mesh: data: 16 (over z, y, x, core).
Axes of the slice: x: 2, y: 2, z: 2, core: 2. Of those that a mesh axis runs over, the one named last changes fastest.
Arguments:
- tokens: bfloat16 [8192, 768], P('data')
- d_logits: bfloat16 [8192, 32000], P('data')
- w_up: bfloat16 [2, 768, 2048], replicated
- w_down: bfloat16 [2, 2048, 768], replicated
- w_out: bfloat16 [768, 32000], replicated
- proj_up: bfloat16 [2, 768, 256], replicated
- proj_down: bfloat16 [2, 768, 256], replicated
- mom_up: float32 [2, 256, 2048], P(None, None, 'data')
- var_up: float32 [2, 256, 2048], P(None, None, 'data')
- mom_down: float32 [2, 2048, 256], P(None, 'data')
- var_down: float32 [2, 2048, 256], P(None, 'data')
- mom_out: float32 [768, 32000], P(None, 'data')
- var_out: float32 [768, 32000], P(None, 'data')
Outputs:
- output 1: bfloat16 [2, 768, 2048], replicated
- output 2: bfloat16 [2, 2048, 768], replicated
- output 3: bfloat16 [768, 32000], replicated
- output 4: float32 [2, 256, 2048], P(None, None, 'data')
- output 5: float32 [2, 256, 2048], P(None, None, 'data')
- output 6: float32 [2, 2048, 256], P(None, 'data')
- output 7: float32 [2, 2048, 256], P(None, 'data')
- output 8: float32 [768, 32000], P(None, 'data')
- output 9: float32 [768, 32000], P(None, 'data')
All inputs are finite; a program needn't handle non-finite values.
Results may differ from the reference program's by a relative error of at most 0.00427494.
Values are sent between devices in bfloat16 or wider.
A program may use at most 1 GiB of HBM per device.

```python
import jax
import jax.numpy as jnp

D = 768
FF = 2048
RANK = 256
VOCAB = 32000
TOKENS = 8192
LAYERS = 2
STEP = 4

BETA1 = 0.9
BETA2 = 0.999
EPS = 1e-8
LR = 0.02
ALPHA = 0.5
LR_HEAD = 0.01


def gelu_tanh(values):
    return jax.nn.gelu(values, approximate=True)


def adam_update(gradient, moment_one, moment_two):
    moment_one = BETA1 * moment_one + (1.0 - BETA1) * gradient
    moment_two = BETA2 * moment_two + (1.0 - BETA2) * gradient * gradient
    direction = (moment_one / (1.0 - BETA1 ** STEP)) / (jnp.sqrt(moment_two / (1.0 - BETA2 ** STEP)) + EPS)
    return moment_one, moment_two, direction


def setup_inputs(seed: int = 0) -> dict:
    subkeys = jax.random.split(jax.random.key(seed), 13)
    scale_up = 0.7 * (D / FF) ** 0.5
    scale_down = 0.85
    scale_out = 1.3 * (D / VOCAB) ** 0.5

    def normal(key_num, arr_dims, factor):
        return jax.random.normal(subkeys[key_num], arr_dims, jnp.float32) * factor

    def spread(key_num, arr_dims, factor):
        return jax.random.uniform(subkeys[key_num], arr_dims, jnp.float32, 0.5, 1.5) * factor

    return {
        'tokens': normal(0, (TOKENS, D), 1.0).astype(jnp.bfloat16),
        'd_logits': normal(1, (TOKENS, VOCAB), (D / (VOCAB * TOKENS)) ** 0.5).astype(jnp.bfloat16),
        'w_up': normal(2, (LAYERS, D, FF), D ** -0.5).astype(jnp.bfloat16),
        'w_down': normal(3, (LAYERS, FF, D), FF ** -0.5).astype(jnp.bfloat16),
        'w_out': normal(4, (D, VOCAB), D ** -0.5).astype(jnp.bfloat16),
        'proj_up': normal(5, (LAYERS, D, RANK), D ** -0.5).astype(jnp.bfloat16),
        'proj_down': normal(6, (LAYERS, D, RANK), D ** -0.5).astype(jnp.bfloat16),
        'mom_up': normal(7, (LAYERS, RANK, FF), 0.1 * scale_up),
        'var_up': spread(8, (LAYERS, RANK, FF), 0.003 * scale_up ** 2),
        'mom_down': normal(9, (LAYERS, FF, RANK), 0.1 * scale_down),
        'var_down': spread(10, (LAYERS, FF, RANK), 0.003 * scale_down ** 2),
        'mom_out': normal(11, (D, VOCAB), 0.1 * scale_out),
        'var_out': spread(12, (D, VOCAB), 0.003 * scale_out ** 2),
    }


def layer_forward(hidden, w_first, w_second):
    pre_act = jnp.dot(hidden, w_first, preferred_element_type=jnp.float32).astype(jnp.bfloat16)
    post_act = gelu_tanh(pre_act.astype(jnp.float32)).astype(jnp.bfloat16)
    new_hidden = (hidden.astype(jnp.float32) + jnp.dot(post_act, w_second, preferred_element_type=jnp.float32)).astype(jnp.bfloat16)
    return new_hidden, pre_act, post_act


def reference(tokens, d_logits, w_up, w_down, w_out, proj_up, proj_down, mom_up, var_up, mom_down, var_down, mom_out, var_out):
    hidden = tokens
    saved_acts = []
    for layer_idx in range(LAYERS):
        new_hidden, pre_act, post_act = layer_forward(hidden, w_up[layer_idx], w_down[layer_idx])
        saved_acts.append((hidden, pre_act, post_act))
        hidden = new_hidden
    grad_head = jnp.dot(hidden.T, d_logits, preferred_element_type=jnp.float32)
    grad_hidden = jnp.dot(d_logits, w_out.T, preferred_element_type=jnp.float32).astype(jnp.bfloat16)
    results = []
    for layer_idx in reversed(range(LAYERS)):
        hidden_in, pre_act, post_act = saved_acts[layer_idx]
        grad_down = jnp.dot(post_act.T, grad_hidden, preferred_element_type=jnp.float32)
        d_post = jnp.dot(grad_hidden, w_down[layer_idx].T, preferred_element_type=jnp.float32)
        gelu_pull = jax.vjp(gelu_tanh, pre_act.astype(jnp.float32))[1]
        d_pre = gelu_pull(d_post)[0].astype(jnp.bfloat16)
        grad_up = jnp.dot(hidden_in.T, d_pre, preferred_element_type=jnp.float32)
        if layer_idx > 0:
            grad_hidden = (grad_hidden.astype(jnp.float32) + jnp.dot(d_pre, w_up[layer_idx].T, preferred_element_type=jnp.float32)).astype(jnp.bfloat16)
        low_up = jnp.dot(proj_up[layer_idx].astype(jnp.float32).T, grad_up, preferred_element_type=jnp.float32)
        low_down = jnp.dot(grad_down, proj_down[layer_idx].astype(jnp.float32), preferred_element_type=jnp.float32)
        m_up, v_up, dir_up = adam_update(low_up, mom_up[layer_idx], var_up[layer_idx])
        m_down, v_down, dir_down = adam_update(low_down, mom_down[layer_idx], var_down[layer_idx])
        step_up = jnp.dot(proj_up[layer_idx], dir_up.astype(jnp.bfloat16), preferred_element_type=jnp.float32)
        step_down = jnp.dot(dir_down.astype(jnp.bfloat16), proj_down[layer_idx].T, preferred_element_type=jnp.float32)
        new_up = (w_up[layer_idx].astype(jnp.float32) - LR * ALPHA * step_up).astype(jnp.bfloat16)
        new_down = (w_down[layer_idx].astype(jnp.float32) - LR * ALPHA * step_down).astype(jnp.bfloat16)
        results.append((new_up, new_down, m_up, v_up, m_down, v_down))
    results = results[::-1]
    m_out, v_out, dir_out = adam_update(grad_head, mom_out, var_out)
    w_out_new = (w_out.astype(jnp.float32) - LR_HEAD * dir_out).astype(jnp.bfloat16)
    return (jnp.stack([entry[0] for entry in results]),
            jnp.stack([entry[1] for entry in results]),
            w_out_new,
            jnp.stack([entry[2] for entry in results]),
            jnp.stack([entry[3] for entry in results]),
            jnp.stack([entry[4] for entry in results]),
            jnp.stack([entry[5] for entry in results]),
            m_out,
            v_out)
```

```python
import jax
import jax.numpy as jnp
from jax import lax
from jax.experimental import pallas as pl
from jax.experimental.pallas import tpu as pltpu
from jax.sharding import PartitionSpec as P


BETA1 = 0.9
BETA2 = 0.999
EPS = 1e-8
STEP = 4
LR = 0.02
ALPHA = 0.5
LR_HEAD = 0.01
DATA_AXIS = 'data'
DEVICES = 16
LANES = 128
CORE, X, Y, Z = 1, 2, 4, 8
GROUP_BITS = ((Z, Y, X), (Y, X, Z), (X, Z, Y))
GROUP_TILES = (6, 5, 5)
ROW_CHUNK = 256


def gelu_tanh(values):
    return jax.nn.gelu(values, approximate=True)


def adam_update(gradient, moment_one, moment_two):
    moment_one = BETA1 * moment_one + (1.0 - BETA1) * gradient
    moment_two = BETA2 * moment_two + (1.0 - BETA2) * gradient * gradient
    direction = (moment_one / (1.0 - BETA1 ** STEP)) / (jnp.sqrt(moment_two / (1.0 - BETA2 ** STEP)) + EPS)
    return moment_one, moment_two, direction


def swap(values, mask):
    return lax.ppermute(values, DATA_AXIS, [(i, i ^ mask) for i in range(DEVICES)])


def group_offsets():
    offsets = [0]
    for tiles in GROUP_TILES:
        offsets.append(offsets[-1] + tiles * LANES)
    return offsets


def pack_columns(values, jobs, shard_cols):
    rows, total = values.shape
    count = jobs[0][0].shape[0]
    row_block = 256
    tables, in_specs, out_specs, out_shapes = [], [], [], []
    for j, (owners, offset, width) in enumerate(jobs):
        window = width + LANES
        starts = owners * shard_cols + offset
        tiles = starts // LANES
        bases = jnp.minimum(tiles, (total - window) // LANES)
        tables.append(jnp.stack([bases, tiles - bases, starts % LANES]))
        in_specs.append(pl.BlockSpec((pl.Element(rows), pl.Element(window)), lambda s, t, j=j: (0, pl.multiple_of(t[j, 0, s] * LANES, LANES))))
        out_specs.append(pl.BlockSpec((1, rows, width), lambda s, t: (s, 0, 0)))
        out_shapes.append(jax.ShapeDtypeStruct((count, rows, width), jnp.bfloat16))

    def body(table_ref, *refs):
        entry = pl.program_id(0)

        def selector(depth, cols, by):
            source = lax.broadcasted_iota(jnp.int32, (depth, cols), 0)
            target = lax.broadcasted_iota(jnp.int32, (depth, cols), 1)
            return jnp.where(source == target + by, 1.0, 0.0).astype(jnp.bfloat16)

        for j, (_, _, width) in enumerate(jobs):
            in_ref, out_ref = refs[j], refs[len(jobs) + j]
            first, shift = table_ref[j, 1, entry], table_ref[j, 2, entry]
            tail = width % (2 * LANES) or 2 * LANES
            inner = selector(3 * LANES, 2 * LANES, shift)
            outer = selector(tail + LANES, tail, shift + first * LANES)

            def step(i, carry):
                sl = pl.ds(pl.multiple_of(i * row_block, row_block), row_block)
                for at in range(0, width - tail, 2 * LANES):
                    source = in_ref[sl, pl.ds(pl.multiple_of(first * LANES + at, LANES), 3 * LANES)]
                    out_ref[0, sl, at:at + 2 * LANES] = jnp.dot(source, inner, preferred_element_type=jnp.float32).astype(jnp.bfloat16)
                at = width - tail
                out_ref[0, sl, at:] = jnp.dot(in_ref[sl, at:], outer, preferred_element_type=jnp.float32).astype(jnp.bfloat16)
                return carry

            lax.fori_loop(0, rows // row_block, step, 0)

    moved = sum(count * rows * width for _, _, width in jobs)
    return pl.pallas_call(
        body,
        grid_spec=pltpu.PrefetchScalarGridSpec(num_scalar_prefetch=1, grid=(count,), in_specs=in_specs, out_specs=out_specs),
        out_shape=out_shapes,
        cost_estimate=pl.CostEstimate(flops=moved * 768, bytes_accessed=moved * 4, transcendentals=0),
        name='pack_columns',
    )(jnp.stack(tables), *[values] * len(jobs))


def project_gradients(terms, owners):
    count = len(terms)
    model, rank = terms[0][0].shape
    tokens, hidden = terms[0][2].shape
    cols = hidden // owners
    step_owners = 4
    block = step_owners * cols

    def body(*refs):
        out_ref, turned = refs[-2], refs[-1]
        for m in range(count):
            p_ref, h_ref, e_ref = refs[3 * m:3 * m + 3]

            @pl.when(pl.program_id(0) == m)
            def _():
                @pl.when(pl.program_id(1) == 0)
                def _():
                    turned[...] = h_ref[...].T

                gradient = jnp.dot(turned[...], e_ref[...], preferred_element_type=jnp.float32)
                high = gradient.astype(jnp.bfloat16)
                low = (gradient - high.astype(jnp.float32)).astype(jnp.bfloat16)
                left = p_ref[...]
                total = jnp.dot(left, high, preferred_element_type=jnp.float32) + jnp.dot(left, low, preferred_element_type=jnp.float32)
                for k in range(step_owners):
                    out_ref[k, 0] = total[:, k * cols:(k + 1) * cols]

    in_specs, operands = [], []
    for m, (p, h, e) in enumerate(terms):
        in_specs += [pl.BlockSpec((rank, model), lambda t, c: (0, 0)), pl.BlockSpec((tokens, model), lambda t, c: (0, 0)),
                     pl.BlockSpec((tokens, block), lambda t, c, m=m: (0, jnp.where(t == m, c, jnp.where(t < m, 0, hidden // block - 1))))]
        operands += [p.T, h, e]
    return pl.pallas_call(
        body,
        grid=(count, hidden // block),
        in_specs=in_specs,
        out_specs=pl.BlockSpec((step_owners, 1, rank, cols), lambda t, c: (c, t, 0, 0)),
        out_shape=jax.ShapeDtypeStruct((owners, count, rank, cols), jnp.float32),
        scratch_shapes=[pltpu.VMEM((model, tokens), jnp.bfloat16)],
        cost_estimate=pl.CostEstimate(flops=count * 2 * model * hidden * (tokens + 2 * rank), bytes_accessed=count * hidden * (tokens * 2 + rank * 4), transcendentals=0),
        name='project_gradients',
    )(*operands)


def reduce_head(near, packed, w_own, mom_out, var_out, chunk):
    groups = len(GROUP_BITS)
    offsets = group_offsets()
    shard_cols = mom_out.shape[0]
    owners, tokens, _ = packed[0][0].shape
    widths = [offsets[g + 1] - offsets[g] for g in range(groups)]
    masks = [(0, CORE, bit, bit | CORE) for bit, _, _ in GROUP_BITS]
    near_keys = sorted(near)

    def body(*refs):
        near_refs = dict(zip(near_keys, refs))
        refs = refs[len(near_keys):]
        packed_refs = [refs[4 * g:4 * g + 4] for g in range(groups)]
        refs = refs[4 * groups:]
        w_ref, mom_ref, var_ref, w_out_ref, mom_out_ref, var_out_ref = refs[:6]
        refs = refs[6:]
        blocks, refs = refs[:groups], refs[groups:]
        part, refs = refs[:groups], refs[groups:]
        got, refs = refs[:groups], refs[groups:]
        got_own, refs = refs[:groups], refs[groups:]
        w_buf, mom_buf, var_buf, mom_turned, var_turned, load_sem, first_send, first_recv, second_send, second_recv, state_sem = refs
        me = lax.axis_index(DATA_AXIS)
        barrier = pltpu.get_barrier_semaphore()
        for bit in (X, Y, Z):
            pl.semaphore_signal(barrier, inc=1, device_id=(me ^ bit,), device_id_type=pl.DeviceIdType.MESH)

        def load(g, entry):
            return [pltpu.make_async_copy(packed_refs[g][k].at[entry], blocks[g].at[k], load_sem.at[g, k]) for k in range(4)]

        for g in range(groups):
            for copy in load(g, 3):
                copy.start()
        rows = pl.ds(chunk * ROW_CHUNK, ROW_CHUNK)
        valid = pl.ds(0, shard_cols)
        state = [pltpu.make_async_copy(w_ref.at[rows], w_buf, state_sem.at[0]),
                 pltpu.make_async_copy(mom_ref.at[:, rows], mom_turned.at[valid], state_sem.at[1]),
                 pltpu.make_async_copy(var_ref.at[:, rows], var_turned.at[valid], state_sem.at[2])]
        for copy in state:
            copy.start()
        pl.semaphore_wait(barrier, 3)

        def first_copy(g, entry):
            return pltpu.make_async_remote_copy(
                src_ref=part[g].at[entry], dst_ref=got[g].at[entry - 2], send_sem=first_send.at[g, entry - 2], recv_sem=first_recv.at[g, entry - 2],
                device_id=(me ^ GROUP_BITS[g][1],), device_id_type=pl.DeviceIdType.MESH)

        def second_copy(g):
            return pltpu.make_async_remote_copy(
                src_ref=part[g].at[1], dst_ref=got_own[g], send_sem=second_send.at[g], recv_sem=second_recv.at[g],
                device_id=(me ^ GROUP_BITS[g][2],), device_id_type=pl.DeviceIdType.MESH)

        def step(i, carry):
            entry = 3 - i
            for g in range(groups):
                for copy in load(g, entry):
                    copy.wait()
                acc = None
                for k in range(4):
                    term = jnp.dot(near_refs[masks[g][k]][...], blocks[g][k], preferred_element_type=jnp.float32)
                    acc = term if acc is None else acc + term
                part[g][entry] = acc

                @pl.when(i < 3)
                def _():
                    for copy in load(g, entry - 1):
                        copy.start()

                @pl.when(i == 0)
                def _():
                    first_copy(g, 3).start()

                @pl.when(i == 1)
                def _():
                    first_copy(g, 2).start()

                @pl.when(i == 2)
                def _():
                    first_copy(g, 3).wait_recv()
                    part[g][1] = part[g][1] + got[g][1]
                    second_copy(g).start()
            return carry

        lax.fori_loop(0, 4, step, 0)

        for copy in state:
            copy.wait()
        for at in range(0, offsets[-1], LANES):
            cols = slice(at, at + LANES)
            mom_buf[:, cols] = mom_turned[cols].T
            var_buf[:, cols] = var_turned[cols].T
        block = 32
        for g in range(groups):
            first_copy(g, 2).wait_recv()
            second_copy(g).wait_recv()
            cols = slice(offsets[g], offsets[g + 1])

            def adam(i, carry):
                sl = pl.ds(pl.multiple_of(i * block, block), block)
                gradient = part[g][0, sl] + got[g][0, sl] + got_own[g][sl]
                m_new, v_new, direction = adam_update(gradient, mom_buf[sl, cols], var_buf[sl, cols])
                mom_buf[sl, cols] = m_new
                var_buf[sl, cols] = v_new
                w_buf[sl, cols] = (w_buf[sl, cols].astype(jnp.float32) - LR_HEAD * direction).astype(jnp.bfloat16)
                return carry

            lax.fori_loop(0, ROW_CHUNK // block, adam, 0)
        results = [pltpu.make_async_copy(w_buf, w_out_ref, state_sem.at[0]),
                   pltpu.make_async_copy(mom_turned.at[valid], mom_out_ref, state_sem.at[1]),
                   pltpu.make_async_copy(var_turned.at[valid], var_out_ref, state_sem.at[2])]
        results[0].start()
        for at in range(0, offsets[-1], LANES):
            cols = slice(at, at + LANES)
            mom_turned[cols] = mom_buf[:, cols].T
            var_turned[cols] = var_buf[:, cols].T
        results[1].start()
        results[2].start()
        for g in range(groups):
            first_copy(g, 3).wait_send()
            first_copy(g, 2).wait_send()
            second_copy(g).wait_send()
        for copy in results:
            copy.wait()

    anywhere = pl.BlockSpec(memory_space=pl.ANY)
    near_spec = pl.BlockSpec((ROW_CHUNK, tokens), lambda s: (chunk, 0))
    scratch = [pltpu.VMEM((4, tokens, w), jnp.bfloat16) for w in widths]
    scratch += [pltpu.VMEM((owners, ROW_CHUNK, w), jnp.float32) for w in widths]
    scratch += [pltpu.VMEM((2, ROW_CHUNK, w), jnp.float32) for w in widths]
    scratch += [pltpu.VMEM((ROW_CHUNK, w), jnp.float32) for w in widths]
    scratch += [pltpu.VMEM((ROW_CHUNK, offsets[-1]), jnp.bfloat16)]
    scratch += [pltpu.VMEM((ROW_CHUNK, offsets[-1]), jnp.float32)] * 2 + [pltpu.VMEM((offsets[-1], ROW_CHUNK), jnp.float32)] * 2
    scratch += [pltpu.SemaphoreType.DMA((groups, 4)), pltpu.SemaphoreType.DMA((groups, 2)), pltpu.SemaphoreType.DMA((groups, 2)),
                pltpu.SemaphoreType.DMA((groups,)), pltpu.SemaphoreType.DMA((groups,)), pltpu.SemaphoreType.DMA((3,))]
    return pl.pallas_call(
        body,
        grid=(1,),
        in_specs=[near_spec] * len(near_keys) + [anywhere] * (4 * groups + 3),
        out_specs=[anywhere] * 3,
        out_shape=[jax.ShapeDtypeStruct((ROW_CHUNK, offsets[-1]), jnp.bfloat16)] + [jax.ShapeDtypeStruct((shard_cols, ROW_CHUNK), jnp.float32)] * 2,
        scratch_shapes=scratch,
        cost_estimate=pl.CostEstimate(flops=60_000_000_000, bytes_accessed=100_000_000, transcendentals=0),
        compiler_params=pltpu.CompilerParams(collective_id=chunk, has_side_effects=True, vmem_limit_bytes=60 * 1024 * 1024),
        name='reduce_head',
    )(*[near[k] for k in near_keys], *[packed[g][m] for g in range(groups) for m in masks[g]], w_own, mom_out, var_out)


def place_parts(parts, vocab, total_rows, row_chunk, previous):
    shard_cols = vocab // DEVICES
    rows = 32
    count = -(-shard_cols // LANES)

    def body(*refs):
        part_ref, out_ref = refs[0], refs[-1]
        lane = lax.broadcasted_iota(jnp.int32, (rows, LANES), 1)
        pending = None
        for owner in range(DEVICES):
            base, shift = divmod(owner * shard_cols, LANES)
            rolled = []
            for index in range(count):
                piece = part_ref[owner, :, index * LANES:(index + 1) * LANES]
                rolled.append(pltpu.roll(piece, shift, 1) if shift else piece)
            end = owner * shard_cols + shard_cols
            for tile in range(base, -(-end // LANES)):
                index = tile - base
                if shift == 0:
                    value = rolled[index]
                elif index == 0:
                    value = jnp.where(lane < shift, pending, rolled[0])
                elif index == count:
                    value = rolled[count - 1]
                else:
                    value = jnp.where(lane < shift, rolled[index - 1], rolled[index])
                if (tile + 1) * LANES <= end:
                    out_ref[:, tile * LANES:(tile + 1) * LANES] = value
                else:
                    pending = value

    steps = ROW_CHUNK // rows
    in_specs = [pl.BlockSpec((DEVICES, rows, count * LANES), lambda s: (0, s, 0))]
    operands = [parts]
    aliases = {}
    if previous is not None:
        in_specs.append(pl.BlockSpec(memory_space=pl.ANY))
        operands.append(previous)
        aliases = {1: 0}
    return pl.pallas_call(
        body,
        grid=(steps,),
        in_specs=in_specs,
        out_specs=pl.BlockSpec((rows, vocab), lambda s: (row_chunk * steps + s, 0)),
        out_shape=jax.ShapeDtypeStruct((total_rows, vocab), jnp.bfloat16),
        input_output_aliases=aliases,
        cost_estimate=pl.CostEstimate(flops=ROW_CHUNK * vocab * 16, bytes_accessed=ROW_CHUNK * vocab * 4, transcendentals=0),
        name='place_parts',
    )(*operands)


def back_project(gathered, w_up, w_down, proj_up, proj_down):
    layers, model, hidden = w_up.shape
    _, _, rank, cols = gathered.shape
    step_owners = 4
    block = step_owners * cols

    def body(up_dir_ref, down_dir_ref, w_up_ref, w_down_ref, p_ref, q_ref, up_ref, down_ref):
        up_dir = jnp.concatenate([up_dir_ref[k, 0] for k in range(step_owners)], axis=1)
        down_dir = jnp.concatenate([down_dir_ref[k, 0] for k in range(step_owners)], axis=1)
        step_up = jnp.dot(p_ref[0], up_dir, preferred_element_type=jnp.float32)
        up_ref[0] = (w_up_ref[0].astype(jnp.float32) - LR * ALPHA * step_up).astype(jnp.bfloat16)
        step_down = lax.dot_general(down_dir, q_ref[0], (((0,), (1,)), ((), ())), preferred_element_type=jnp.float32)
        down_ref[0] = (w_down_ref[0].astype(jnp.float32) - LR * ALPHA * step_down).astype(jnp.bfloat16)

    up_spec = pl.BlockSpec((1, model, block), lambda l, c: (l, 0, c))
    down_spec = pl.BlockSpec((1, block, model), lambda l, c: (l, c, 0))
    proj_spec = pl.BlockSpec((1, model, rank), lambda l, c: (l, 0, 0))
    return pl.pallas_call(
        body,
        grid=(layers, hidden // block),
        in_specs=[pl.BlockSpec((step_owners, 1, rank, cols), lambda l, c: (c, l, 0, 0)),
                  pl.BlockSpec((step_owners, 1, rank, cols), lambda l, c: (c, layers + l, 0, 0)),
                  up_spec, down_spec, proj_spec, proj_spec],
        out_specs=[up_spec, down_spec],
        out_shape=[jax.ShapeDtypeStruct(w_up.shape, jnp.bfloat16), jax.ShapeDtypeStruct(w_down.shape, jnp.bfloat16)],
        cost_estimate=pl.CostEstimate(flops=8 * model * hidden * rank, bytes_accessed=30_000_000, transcendentals=0),
        name='back_project',
    )(gathered, gathered, w_up, w_down, proj_up, proj_down)


def forward(tokens, w_up, w_down):
    num_layers = w_up.shape[0]
    hidden = tokens
    saved_acts = []
    for layer_idx in range(num_layers):
        pre_act = jnp.dot(hidden, w_up[layer_idx], preferred_element_type=jnp.float32).astype(jnp.bfloat16)
        post_act = gelu_tanh(pre_act.astype(jnp.float32)).astype(jnp.bfloat16)
        saved_acts.append((hidden, pre_act, post_act))
        hidden = (hidden.astype(jnp.float32) + jnp.dot(post_act, w_down[layer_idx], preferred_element_type=jnp.float32)).astype(jnp.bfloat16)
    return hidden, saved_acts


def backward(saved_acts, d_logits, w_up, w_down, w_out):
    num_layers = w_up.shape[0]
    grad_hidden = jnp.einsum('tv,dv->td', d_logits, w_out, preferred_element_type=jnp.float32).astype(jnp.bfloat16)
    up_terms = [None] * num_layers
    down_terms = [None] * num_layers
    for layer_idx in reversed(range(num_layers)):
        hidden_in, pre_act, post_act = saved_acts[layer_idx]
        down_terms[layer_idx] = (grad_hidden, post_act)
        d_post = jnp.einsum('td,fd->tf', grad_hidden, w_down[layer_idx], preferred_element_type=jnp.float32)
        gelu_pull = jax.vjp(gelu_tanh, pre_act.astype(jnp.float32))[1]
        d_pre = gelu_pull(d_post)[0].astype(jnp.bfloat16)
        up_terms[layer_idx] = (hidden_in, d_pre)
        if layer_idx > 0:
            grad_hidden = (grad_hidden.astype(jnp.float32) + jnp.einsum('tf,df->td', d_pre, w_up[layer_idx], preferred_element_type=jnp.float32)).astype(jnp.bfloat16)
    return up_terms, down_terms


def exchange_hidden(hidden):
    near = {0: hidden.T}
    near[CORE] = swap(near[0], CORE)
    for bit in (Z, Y, X):
        near[bit] = swap(near[0], bit)
    for bit in (Z, Y, X):
        near[bit | CORE] = swap(near[bit], CORE)
    return near


def local_step(tokens, d_logits, w_up, w_down, w_out, proj_up, proj_down, mom_up, var_up, mom_down, var_down, mom_out, var_out):
    me = lax.axis_index(DATA_AXIS)
    layers = w_up.shape[0]
    total_rows, vocab = w_out.shape
    shard_cols = mom_out.shape[1]
    offsets = group_offsets()
    mine = {}
    for partner in (2, 3, 1, 0):
        jobs, masks = [], []
        for g, (bit, first, second) in enumerate(GROUP_BITS):
            masks.append((0, CORE, bit, bit | CORE)[partner])
            rels = jnp.array([0, second, first, first | second], jnp.int32) ^ masks[-1]
            jobs.append((rels ^ me, offsets[g], offsets[g + 1] - offsets[g]))
        for g, value in enumerate(pack_columns(d_logits, jobs, shard_cols)):
            mine[g, masks[g]] = value
    packed = [dict() for _ in GROUP_BITS]
    for (g, mask), value in mine.items():
        packed[g][mask] = swap(value, mask) if mask else value
    tokens, mine = lax.optimization_barrier((tokens, mine))
    hidden, saved_acts = forward(tokens, w_up, w_down)
    near = exchange_hidden(hidden)
    up_terms, down_terms = backward(saved_acts, d_logits, w_up, w_down, w_out)
    terms = [(proj_up[l], *up_terms[l]) for l in range(layers)] + [(proj_down[l], *down_terms[l]) for l in range(layers)]
    low = project_gradients(terms, DEVICES)
    _, _, rank, cols = low.shape
    low_scattered = lax.psum_scatter(low.reshape(-1, cols), DATA_AXIS, scatter_dimension=0, tiled=True).reshape(2 * layers, rank, cols)
    w_own = pack_columns(w_out, [(me[None], 0, offsets[-1])], shard_cols)[0][0]
    w_own, near, low = lax.optimization_barrier((w_own, near, low))
    chunks = total_rows // ROW_CHUNK
    results = []
    gathered = []
    for chunk in range(chunks):
        if results:
            w_own, results[-1][0] = lax.optimization_barrier((w_own, results[-1][0]))
        results.append(list(reduce_head(near, packed, w_own, mom_out.T, var_out.T, chunk)))
        payload = results[-1][0]
        if chunk == 1:
            low_scattered, payload = lax.optimization_barrier((low_scattered, payload))
            m_up, v_up, dir_up = adam_update(low_scattered[:layers], mom_up, var_up)
            m_down, v_down, dir_down = adam_update(low_scattered[layers:].transpose(0, 2, 1), mom_down, var_down)
            dirs = jnp.concatenate([dir_up, dir_down.transpose(0, 2, 1)], axis=0).astype(jnp.bfloat16)
            side = payload.shape[1] // cols
            dirs = dirs.reshape(side, -1, cols).transpose(1, 0, 2).reshape(-1, payload.shape[1])
            payload = jnp.concatenate([payload, dirs], axis=0)
        gathered.append(lax.all_gather(payload, DATA_AXIS, axis=0))
    w_out_new = None
    gathered[0], results[-1][1] = lax.optimization_barrier((gathered[0], results[-1][1]))
    for chunk in range(chunks):
        w_out_new = place_parts(gathered[chunk], vocab, total_rows, chunk, w_out_new)
    dirs = gathered[1][:, ROW_CHUNK:].reshape(DEVICES, -1, side, cols).transpose(0, 2, 1, 3).reshape(DEVICES, 2 * layers, rank, cols)
    w_up_new, w_down_new = back_project(dirs, w_up, w_down, proj_up, proj_down)
    m_out = jnp.concatenate([r[1] for r in results], axis=1).T
    v_out = jnp.concatenate([r[2] for r in results], axis=1).T
    return w_up_new, w_down_new, w_out_new, m_up, v_up, m_down, v_down, m_out, v_out


def solution(mesh):
    row_spec = P(DATA_AXIS, None)
    whole = P()
    up_spec = P(None, None, DATA_AXIS)
    down_spec = P(None, DATA_AXIS, None)
    head_spec = P(None, DATA_AXIS)
    in_specs = (row_spec, row_spec, whole, whole, whole, whole, whole, up_spec, up_spec, down_spec, down_spec, head_spec, head_spec)
    out_specs = (whole, whole, whole, up_spec, up_spec, down_spec, down_spec, head_spec, head_spec)

    return jax.shard_map(local_step, mesh=mesh, in_specs=in_specs, out_specs=out_specs, check_vma=False)
```

```python
import jax
import jax.numpy as jnp
from jax import lax
from jax.experimental import pallas as pl
from jax.experimental.pallas import tpu as pltpu
from jax.sharding import PartitionSpec as P


BETA1 = 0.9
BETA2 = 0.999
EPS = 1e-8
STEP = 4
LR = 0.02
ALPHA = 0.5
LR_HEAD = 0.01
DATA_AXIS = 'data'
DEVICES = 16
LANES = 128
CORE, X, Y, Z = 1, 2, 4, 8
GROUP_BITS = ((Z, Y, X), (Y, X, Z), (X, Z, Y))
GROUP_TILES = (6, 5, 5)
TERM_BITS = ((X, Y, Z), (Y, Z, X), (Z, X, Y), (Z, Y, X))
LOW_STEPS = 2
PACKS = (((0, 2),), ((1, 2), (2, 2)), ((0, 3), (1, 3), (2, 3)), ((0, 1), (1, 1), (2, 1)), ((0, 0), (1, 0), (2, 0)))
ROW_CHUNKS = (256, 256, 256)


def gelu_tanh(values):
    return jax.nn.gelu(values, approximate=True)


def adam_update(gradient, moment_one, moment_two):
    moment_one = BETA1 * moment_one + (1.0 - BETA1) * gradient
    moment_two = BETA2 * moment_two + (1.0 - BETA2) * gradient * gradient
    direction = (moment_one / (1.0 - BETA1 ** STEP)) / (jnp.sqrt(moment_two / (1.0 - BETA2 ** STEP)) + EPS)
    return moment_one, moment_two, direction


def swap(values, mask):
    return lax.ppermute(values, DATA_AXIS, [(i, i ^ mask) for i in range(DEVICES)])


def partner_mask(group, partner):
    bit = GROUP_BITS[group][0]
    return (0, CORE, bit, bit | CORE)[partner]


def group_offsets():
    offsets = [0]
    for tiles in GROUP_TILES:
        offsets.append(offsets[-1] + tiles * LANES)
    return offsets


def shift_left(ref, rows, first, tiles, shift, lane):
    last = ref.shape[1] // LANES - 1

    def rolled(index):
        at = pl.multiple_of(jnp.minimum(first + index, last) * LANES, LANES)
        return pltpu.roll(ref[rows, pl.ds(at, LANES)], (LANES - shift) % LANES, 1)

    pieces = []
    left = rolled(0)
    for index in range(tiles):
        right = rolled(index + 1)
        pieces.append(jnp.where(lane < LANES - shift, left, right))
        left = right
    return pieces


def pack_columns(values, jobs, shard_cols):
    rows, total = values.shape
    count = jobs[0][0].shape[0]
    row_block = 256
    tables, in_specs, out_specs, out_shapes = [], [], [], []
    for j, (owners, offset, width) in enumerate(jobs):
        window = width + LANES
        starts = owners * shard_cols + offset
        tiles = starts // LANES
        bases = jnp.minimum(tiles, (total - window) // LANES)
        tables.append(jnp.stack([bases, tiles - bases, starts % LANES]))
        in_specs.append(pl.BlockSpec((pl.Element(rows), pl.Element(window)), lambda s, t, j=j: (0, pl.multiple_of(t[j, 0, s] * LANES, LANES))))
        out_specs.append(pl.BlockSpec((1, rows, width), lambda s, t: (s, 0, 0)))
        out_shapes.append(jax.ShapeDtypeStruct((count, rows, width), jnp.bfloat16))

    def body(table_ref, *refs):
        entry = pl.program_id(0)

        def selector(depth, cols, by):
            source = lax.broadcasted_iota(jnp.int32, (depth, cols), 0)
            target = lax.broadcasted_iota(jnp.int32, (depth, cols), 1)
            return jnp.where(source == target + by, 1.0, 0.0).astype(jnp.bfloat16)

        plans = []
        for j, (_, _, width) in enumerate(jobs):
            first, shift = table_ref[j, 1, entry], table_ref[j, 2, entry]
            tail = width % (2 * LANES) or 2 * LANES
            by_roll = len(jobs) > 2 and j == len(jobs) - 1
            selectors = None if by_roll else (selector(3 * LANES, 2 * LANES, shift), selector(tail + LANES, tail, shift + first * LANES))
            plans.append((refs[j], refs[len(jobs) + j], width, tail, first, shift, selectors))
        lane = lax.broadcasted_iota(jnp.int32, (row_block, LANES), 1)

        def step(i, carry):
            sl = pl.ds(pl.multiple_of(i * row_block, row_block), row_block)
            for in_ref, out_ref, width, tail, first, shift, selectors in plans:
                if selectors is None:
                    for t, piece in enumerate(shift_left(in_ref, sl, first, width // LANES, shift, lane)):
                        out_ref[0, sl, t * LANES:(t + 1) * LANES] = piece
                    continue
                inner, outer = selectors
                for at in range(0, width - tail, 2 * LANES):
                    source = in_ref[sl, pl.ds(pl.multiple_of(first * LANES + at, LANES), 3 * LANES)]
                    out_ref[0, sl, at:at + 2 * LANES] = jnp.dot(source, inner, preferred_element_type=jnp.float32).astype(jnp.bfloat16)
                at = width - tail
                out_ref[0, sl, at:] = jnp.dot(in_ref[sl, at:], outer, preferred_element_type=jnp.float32).astype(jnp.bfloat16)
            return carry

        lax.fori_loop(0, rows // row_block, step, 0)

    moved = sum(count * rows * width for _, _, width in jobs)
    return pl.pallas_call(
        body,
        grid_spec=pltpu.PrefetchScalarGridSpec(num_scalar_prefetch=1, grid=(count,), in_specs=in_specs, out_specs=out_specs),
        out_shape=out_shapes,
        cost_estimate=pl.CostEstimate(flops=moved * 768, bytes_accessed=moved * 4, transcendentals=0),
        name='pack_columns',
    )(jnp.stack(tables), *[values] * len(jobs))


def project_gradients(terms, owners, me):
    count = len(terms)
    model, rank = terms[0][0].shape
    tokens, hidden = terms[0][2].shape
    cols = hidden // owners
    step_owners = 8
    block = step_owners * cols

    rel = jnp.arange(owners, dtype=jnp.int32) ^ me
    table = jnp.stack([sum(jnp.where(rel & bit, owners >> (k + 1), 0) for k, bit in enumerate((CORE, *bits))) for bits in TERM_BITS])

    def body(table_ref, *refs):
        out_ref, turned = refs[-2], refs[-1]
        for m in range(count):
            p_ref, h_ref, e_ref = refs[3 * m:3 * m + 3]

            @pl.when(pl.program_id(0) == m)
            def _():
                @pl.when(pl.program_id(1) == 0)
                def _():
                    turned[...] = h_ref[...].T

                gradient = jnp.dot(turned[...], e_ref[...], preferred_element_type=jnp.float32)
                high = gradient.astype(jnp.bfloat16)
                low = (gradient - high.astype(jnp.float32)).astype(jnp.bfloat16)
                left = p_ref[...]
                total = jnp.dot(left, high, preferred_element_type=jnp.float32) + jnp.dot(left, low, preferred_element_type=jnp.float32)
                for k in range(step_owners):
                    out_ref[0, table_ref[m, pl.program_id(1) * step_owners + k]] = total[:, k * cols:(k + 1) * cols]

    in_specs, operands = [], []
    for m, (p, h, e) in enumerate(terms):
        in_specs += [pl.BlockSpec((rank, model), lambda t, c, _: (0, 0)), pl.BlockSpec((tokens, model), lambda t, c, _: (0, 0)),
                     pl.BlockSpec((tokens, block), lambda t, c, _, m=m: (0, jnp.where(t == m, c, jnp.where(t < m, 0, hidden // block - 1))))]
        operands += [p.T, h, e]
    return pl.pallas_call(
        body,
        grid_spec=pltpu.PrefetchScalarGridSpec(
            num_scalar_prefetch=1,
            grid=(count, hidden // block),
            in_specs=in_specs,
            out_specs=pl.BlockSpec((1, owners, rank, cols), lambda t, c, _: (t, 0, 0, 0)),
            scratch_shapes=[pltpu.VMEM((model, tokens), jnp.bfloat16)],
        ),
        out_shape=jax.ShapeDtypeStruct((count, owners, rank, cols), jnp.float32),
        cost_estimate=pl.CostEstimate(flops=count * 2 * model * hidden * (tokens + 2 * rank), bytes_accessed=count * hidden * (tokens * 2 + rank * 4), transcendentals=0),
        name='project_gradients',
    )(table, *operands)


def reduce_head(near, packed, w_out, mom_out, var_out, chunk, low=None):
    groups = len(GROUP_BITS)
    offsets = group_offsets()
    row_chunk = ROW_CHUNKS[chunk]
    places = 0 if low is None else low.shape[1]
    last_tile = (w_out.shape[1] - offsets[-1] - LANES) // LANES
    shard_cols = mom_out.shape[0]
    owners, tokens, _ = packed[0][0].shape
    widths = [offsets[g + 1] - offsets[g] for g in range(groups)]
    masks = [(0, CORE, bit, bit | CORE) for bit, _, _ in GROUP_BITS]
    near_keys = sorted(near)

    def body(*refs):
        near_refs = dict(zip(near_keys, refs))
        refs = refs[len(near_keys):]
        if low is not None:
            low_ref, refs = refs[0], refs[1:]
        packed_refs = [refs[4 * g:4 * g + 4] for g in range(groups)]
        refs = refs[4 * groups:]
        w_ref, mom_ref, var_ref, w_out_ref, mom_out_ref, var_out_ref = refs[:6]
        refs = refs[6:]
        if low is not None:
            low_out_ref, low_buf, *low_got, low_load, low_send, low_recv = refs[:5 + LOW_STEPS]
            refs = refs[5 + LOW_STEPS:]
        near_buf, near_sem, w_window, *refs = refs
        blocks, refs = refs[:groups], refs[groups:]
        part, refs = refs[:groups], refs[groups:]
        got, refs = refs[:groups], refs[groups:]
        got_own, refs = refs[:groups], refs[groups:]
        w_buf, mom_buf, var_buf, mom_turned, var_turned, load_sem, first_send, first_recv, second_send, second_recv, state_sem = refs
        me = lax.axis_index(DATA_AXIS)
        barrier = pltpu.get_barrier_semaphore()
        greeted = (X, Y, Z, CORE) if low is not None and chunk == 0 else (X, Y, Z)
        for bit in greeted:
            pl.semaphore_signal(barrier, inc=1, device_id=(me ^ bit,), device_id_type=pl.DeviceIdType.MESH)

        def load(g, entry):
            return [pltpu.make_async_copy(packed_refs[g][k].at[entry], blocks[g].at[k], load_sem.at[g, k]) for k in range(4)]

        for g in range(groups):
            for copy in load(g, 3):
                copy.start()
        rows = pl.ds(sum(ROW_CHUNKS[:chunk]), row_chunk)
        valid = pl.ds(0, shard_cols)
        own_tile = (me * shard_cols) // LANES
        base_tile = jnp.minimum(own_tile, last_tile)
        window = pl.ds(pl.multiple_of(base_tile * LANES, LANES), offsets[-1] + LANES)
        state = [pltpu.make_async_copy(w_ref.at[rows, window], w_window, state_sem.at[0]),
                 pltpu.make_async_copy(mom_ref.at[:, rows], mom_turned.at[valid], state_sem.at[1]),
                 pltpu.make_async_copy(var_ref.at[:, rows], var_turned.at[valid], state_sem.at[2])]
        near_loads = [pltpu.make_async_copy(near_refs[masks[g][k]].at[rows], near_buf.at[g, k], near_sem.at[g, k]) for g in range(groups) for k in range(4)]
        for copy in near_loads:
            copy.start()
        for copy in state:
            copy.start()
        pl.semaphore_wait(barrier, len(greeted))

        def low_copy(at, term):
            half = places >> (at + 1)
            source = low_ref if at == 0 else low_buf
            return pltpu.make_async_remote_copy(
                src_ref=source.at[term, pl.ds(half, half)], dst_ref=low_got[at].at[term], send_sem=low_send.at[at, term], recv_sem=low_recv.at[at, term],
                device_id=(me ^ (CORE, *TERM_BITS[term])[chunk * LOW_STEPS + at],), device_id_type=pl.DeviceIdType.MESH)

        def low_step(at):
            half = places >> (at + 1)
            for term in range(len(TERM_BITS)):
                low_copy(at, term).wait_recv()

                def add(e, carry):
                    low_buf[term, e] = low_buf[term, e] + low_got[at][term, e]
                    return carry

                lax.fori_loop(0, half, add, 0)
                if at + 1 < LOW_STEPS:
                    low_copy(at + 1, term).start()

        if low is not None:
            keep = pl.ds(0, places // 2)
            low_loads = [pltpu.make_async_copy(low_ref.at[term, keep], low_buf.at[term], low_load.at[term]) for term in range(len(TERM_BITS))]
            for term, copy in enumerate(low_loads):
                low_copy(0, term).start()
                copy.start()
        for copy in near_loads:
            copy.wait()

        def first_copy(g, entry):
            return pltpu.make_async_remote_copy(
                src_ref=part[g].at[entry], dst_ref=got[g].at[entry - 2], send_sem=first_send.at[g, entry - 2], recv_sem=first_recv.at[g, entry - 2],
                device_id=(me ^ GROUP_BITS[g][1],), device_id_type=pl.DeviceIdType.MESH)

        def second_copy(g):
            return pltpu.make_async_remote_copy(
                src_ref=part[g].at[1], dst_ref=got_own[g], send_sem=second_send.at[g], recv_sem=second_recv.at[g],
                device_id=(me ^ GROUP_BITS[g][2],), device_id_type=pl.DeviceIdType.MESH)

        def step(i, carry):
            entry = 3 - i
            if low is not None:
                @pl.when(i == 1)
                def _():
                    for copy in low_loads:
                        copy.wait()
                    low_step(0)
            for g in range(groups):
                for copy in load(g, entry):
                    copy.wait()

                def accumulate(k, carry):
                    term = jnp.dot(near_buf[g, k], blocks[g][k], preferred_element_type=jnp.float32)

                    @pl.when(k == 0)
                    def _():
                        part[g][entry] = term

                    @pl.when(k > 0)
                    def _():
                        part[g][entry] = part[g][entry] + term

                    return carry

                lax.fori_loop(0, 4, accumulate, 0)

                @pl.when(i < 3)
                def _():
                    for copy in load(g, entry - 1):
                        copy.start()

                @pl.when(i == 0)
                def _():
                    first_copy(g, 3).start()

                @pl.when(i == 1)
                def _():
                    first_copy(g, 2).start()

                @pl.when(i == 2)
                def _():
                    first_copy(g, 3).wait_recv()
                    part[g][1] = part[g][1] + got[g][1]
                    second_copy(g).start()
            return carry

        lax.fori_loop(0, 4, step, 0)

        for copy in state:
            copy.wait()
        lane = lax.broadcasted_iota(jnp.int32, (64, LANES), 1)

        def align(i, carry):
            sl = pl.ds(pl.multiple_of(i * 64, 64), 64)
            for t, piece in enumerate(shift_left(w_window, sl, own_tile - base_tile, offsets[-1] // LANES, (me * shard_cols) % LANES, lane)):
                w_buf[sl, t * LANES:(t + 1) * LANES] = piece
            return carry

        lax.fori_loop(0, row_chunk // 64, align, 0)
        for at in range(0, offsets[-1], LANES):
            cols = slice(at, at + LANES)
            mom_buf[:, cols] = mom_turned[cols].T
            var_buf[:, cols] = var_turned[cols].T
        block = 32
        for g in range(groups):
            first_copy(g, 2).wait_recv()
        for g in range(groups):
            second_copy(g).wait_recv()
            cols = slice(offsets[g], offsets[g + 1])

            def adam(i, carry):
                sl = pl.ds(pl.multiple_of(i * block, block), block)
                gradient = part[g][0, sl] + got[g][0, sl] + got_own[g][sl]
                m_new, v_new, direction = adam_update(gradient, mom_buf[sl, cols], var_buf[sl, cols])
                mom_buf[sl, cols] = m_new
                var_buf[sl, cols] = v_new
                w_buf[sl, cols] = (w_buf[sl, cols].astype(jnp.float32) - LR_HEAD * direction).astype(jnp.bfloat16)
                return carry

            lax.fori_loop(0, row_chunk // block, adam, 0)
        results = [pltpu.make_async_copy(w_buf, w_out_ref, state_sem.at[0]),
                   pltpu.make_async_copy(mom_turned.at[valid], mom_out_ref, state_sem.at[1]),
                   pltpu.make_async_copy(var_turned.at[valid], var_out_ref, state_sem.at[2])]
        results[0].start()
        for at in range(0, offsets[-1], LANES):
            cols = slice(at, at + LANES)
            mom_turned[cols] = mom_buf[:, cols].T
            var_turned[cols] = var_buf[:, cols].T
        results[1].start()
        results[2].start()
        if low is not None:
            low_step(1)
            results += [pltpu.make_async_copy(low_buf.at[term, pl.ds(0, places >> LOW_STEPS)], low_out_ref.at[term], low_load.at[term]) for term in range(len(TERM_BITS))]
            for copy in results[3:]:
                copy.start()
            for at in range(LOW_STEPS):
                for term in range(len(TERM_BITS)):
                    low_copy(at, term).wait_send()
        for g in range(groups):
            first_copy(g, 3).wait_send()
            first_copy(g, 2).wait_send()
            second_copy(g).wait_send()
        for copy in results:
            copy.wait()

    anywhere = pl.BlockSpec(memory_space=pl.ANY)
    out_shapes = [jax.ShapeDtypeStruct((row_chunk, offsets[-1]), jnp.bfloat16)] + [jax.ShapeDtypeStruct((shard_cols, row_chunk), jnp.float32)] * 2
    scratch = []
    if low is not None:
        terms, _, rank, cols = low.shape
        out_shapes.append(jax.ShapeDtypeStruct((terms, places >> LOW_STEPS, rank, cols), jnp.float32))
        scratch.append(pltpu.VMEM((terms, places // 2, rank, cols), jnp.float32))
        scratch += [pltpu.VMEM((terms, places >> (at + 1), rank, cols), jnp.float32) for at in range(LOW_STEPS)]
        scratch += [pltpu.SemaphoreType.DMA((terms,)), pltpu.SemaphoreType.DMA((LOW_STEPS, terms)), pltpu.SemaphoreType.DMA((LOW_STEPS, terms))]
    scratch += [pltpu.VMEM((groups, 4, row_chunk, tokens), jnp.bfloat16), pltpu.SemaphoreType.DMA((groups, 4)), pltpu.VMEM((row_chunk, offsets[-1] + LANES), jnp.bfloat16)]
    scratch += [pltpu.VMEM((4, tokens, w), jnp.bfloat16) for w in widths]
    scratch += [pltpu.VMEM((owners, row_chunk, w), jnp.float32) for w in widths]
    scratch += [pltpu.VMEM((2, row_chunk, w), jnp.float32) for w in widths]
    scratch += [pltpu.VMEM((row_chunk, w), jnp.float32) for w in widths]
    scratch += [pltpu.VMEM((row_chunk, offsets[-1]), jnp.bfloat16)]
    scratch += [pltpu.VMEM((row_chunk, offsets[-1]), jnp.float32)] * 2 + [pltpu.VMEM((offsets[-1], row_chunk), jnp.float32)] * 2
    scratch += [pltpu.SemaphoreType.DMA((groups, 4)), pltpu.SemaphoreType.DMA((groups, 2)), pltpu.SemaphoreType.DMA((groups, 2)),
                pltpu.SemaphoreType.DMA((groups,)), pltpu.SemaphoreType.DMA((groups,)), pltpu.SemaphoreType.DMA((3,))]
    return pl.pallas_call(
        body,
        in_specs=[anywhere] * (len(near_keys) + 4 * groups + 3 + (low is not None)),
        out_specs=[anywhere] * len(out_shapes),
        out_shape=out_shapes,
        scratch_shapes=scratch,
        cost_estimate=pl.CostEstimate(flops=60_000_000_000, bytes_accessed=100_000_000, transcendentals=0),
        compiler_params=pltpu.CompilerParams(collective_id=chunk, has_side_effects=True, vmem_limit_bytes=60 * 1024 * 1024),
        name='reduce_head',
    )(*[near[k] for k in near_keys], *([] if low is None else [low]), *[packed[g][m] for g in range(groups) for m in masks[g]], w_out, mom_out, var_out)


def place_parts(parts, vocab, total_rows, chunk, previous):
    shard_cols = vocab // DEVICES
    rows = 32
    count = -(-shard_cols // LANES)

    def body(*refs):
        part_ref, out_ref = refs[0], refs[-1]
        lane = lax.broadcasted_iota(jnp.int32, (rows, LANES), 1)
        pending = None
        for owner in range(DEVICES):
            base, shift = divmod(owner * shard_cols, LANES)
            rolled = []
            for index in range(count):
                piece = part_ref[owner, :, index * LANES:(index + 1) * LANES]
                rolled.append(pltpu.roll(piece, shift, 1) if shift else piece)
            end = owner * shard_cols + shard_cols
            for tile in range(base, -(-end // LANES)):
                index = tile - base
                if shift == 0:
                    value = rolled[index]
                elif index == 0:
                    value = jnp.where(lane < shift, pending, rolled[0])
                elif index == count:
                    value = rolled[count - 1]
                else:
                    value = jnp.where(lane < shift, rolled[index - 1], rolled[index])
                if (tile + 1) * LANES <= end:
                    out_ref[:, tile * LANES:(tile + 1) * LANES] = value
                else:
                    pending = value

    steps = ROW_CHUNKS[chunk] // rows
    start = sum(ROW_CHUNKS[:chunk]) // rows
    in_specs = [pl.BlockSpec((DEVICES, rows, count * LANES), lambda s: (0, s, 0))]
    operands = [parts]
    aliases = {}
    if previous is not None:
        in_specs.append(pl.BlockSpec(memory_space=pl.ANY))
        operands.append(previous)
        aliases = {1: 0}
    return pl.pallas_call(
        body,
        grid=(steps,),
        in_specs=in_specs,
        out_specs=pl.BlockSpec((rows, vocab), lambda s: (start + s, 0)),
        out_shape=jax.ShapeDtypeStruct((total_rows, vocab), jnp.bfloat16),
        input_output_aliases=aliases,
        cost_estimate=pl.CostEstimate(flops=ROW_CHUNKS[chunk] * vocab * 16, bytes_accessed=ROW_CHUNKS[chunk] * vocab * 4, transcendentals=0),
        name='place_parts',
    )(*operands)


def back_project(gathered, w_up, w_down, proj_up, proj_down):
    layers, model, hidden = w_up.shape
    _, _, rank, cols = gathered.shape
    step_owners = 4
    block = step_owners * cols

    def body(up_dir_ref, down_dir_ref, w_up_ref, w_down_ref, p_ref, q_ref, up_ref, down_ref):
        up_dir = jnp.concatenate([up_dir_ref[k, 0] for k in range(step_owners)], axis=1)
        down_dir = jnp.concatenate([down_dir_ref[k, 0] for k in range(step_owners)], axis=1)
        step_up = jnp.dot(p_ref[0], up_dir, preferred_element_type=jnp.float32)
        up_ref[0] = (w_up_ref[0].astype(jnp.float32) - LR * ALPHA * step_up).astype(jnp.bfloat16)
        step_down = lax.dot_general(down_dir, q_ref[0], (((0,), (1,)), ((), ())), preferred_element_type=jnp.float32)
        down_ref[0] = (w_down_ref[0].astype(jnp.float32) - LR * ALPHA * step_down).astype(jnp.bfloat16)

    up_spec = pl.BlockSpec((1, model, block), lambda l, c: (l, 0, c))
    down_spec = pl.BlockSpec((1, block, model), lambda l, c: (l, c, 0))
    proj_spec = pl.BlockSpec((1, model, rank), lambda l, c: (l, 0, 0))
    return pl.pallas_call(
        body,
        grid=(layers, hidden // block),
        in_specs=[pl.BlockSpec((step_owners, 1, rank, cols), lambda l, c: (c, l, 0, 0)),
                  pl.BlockSpec((step_owners, 1, rank, cols), lambda l, c: (c, layers + l, 0, 0)),
                  up_spec, down_spec, proj_spec, proj_spec],
        out_specs=[up_spec, down_spec],
        out_shape=[jax.ShapeDtypeStruct(w_up.shape, jnp.bfloat16), jax.ShapeDtypeStruct(w_down.shape, jnp.bfloat16)],
        cost_estimate=pl.CostEstimate(flops=8 * model * hidden * rank, bytes_accessed=30_000_000, transcendentals=0),
        name='back_project',
    )(gathered, gathered, w_up, w_down, proj_up, proj_down)


def forward(tokens, w_up, w_down):
    num_layers = w_up.shape[0]
    hidden = tokens
    saved_acts = []
    for layer_idx in range(num_layers):
        pre_act = jnp.dot(hidden, w_up[layer_idx], preferred_element_type=jnp.float32).astype(jnp.bfloat16)
        post_act = gelu_tanh(pre_act.astype(jnp.float32)).astype(jnp.bfloat16)
        saved_acts.append((hidden, pre_act, post_act))
        hidden = (hidden.astype(jnp.float32) + jnp.dot(post_act, w_down[layer_idx], preferred_element_type=jnp.float32)).astype(jnp.bfloat16)
    return hidden, saved_acts


def backward(saved_acts, d_logits, w_up, w_down, w_out):
    num_layers = w_up.shape[0]
    grad_hidden = jnp.einsum('tv,dv->td', d_logits, w_out, preferred_element_type=jnp.float32).astype(jnp.bfloat16)
    up_terms = [None] * num_layers
    down_terms = [None] * num_layers
    for layer_idx in reversed(range(num_layers)):
        hidden_in, pre_act, post_act = saved_acts[layer_idx]
        down_terms[layer_idx] = (grad_hidden, post_act)
        d_post = jnp.einsum('td,fd->tf', grad_hidden, w_down[layer_idx], preferred_element_type=jnp.float32)
        gelu_pull = jax.vjp(gelu_tanh, pre_act.astype(jnp.float32))[1]
        d_pre = gelu_pull(d_post)[0].astype(jnp.bfloat16)
        up_terms[layer_idx] = (hidden_in, d_pre)
        if layer_idx > 0:
            grad_hidden = (grad_hidden.astype(jnp.float32) + jnp.einsum('tf,df->td', d_pre, w_up[layer_idx], preferred_element_type=jnp.float32)).astype(jnp.bfloat16)
    return up_terms, down_terms


def exchange_hidden(hidden):
    near = {0: hidden.T}
    near[CORE] = swap(near[0], CORE)
    for bit in (Z, Y, X):
        near[bit] = swap(near[0], bit)
    for bit in (Z, Y, X):
        near[bit | CORE] = swap(near[bit], CORE)
    return near


def local_step(tokens, d_logits, w_up, w_down, w_out, proj_up, proj_down, mom_up, var_up, mom_down, var_down, mom_out, var_out):
    me = lax.axis_index(DATA_AXIS)
    layers = w_up.shape[0]
    total_rows, vocab = w_out.shape
    shard_cols = mom_out.shape[1]
    offsets = group_offsets()
    mine = {}
    for pack in PACKS:
        jobs, keys = [], []
        for g, partner in pack:
            _, first, second = GROUP_BITS[g]
            mask = partner_mask(g, partner)
            rels = jnp.array([0, second, first, first | second], jnp.int32) ^ mask
            jobs.append((rels ^ me, offsets[g], offsets[g + 1] - offsets[g]))
            keys.append((g, mask))
        for key, value in zip(keys, pack_columns(d_logits, jobs, shard_cols)):
            mine[key] = value
    packed = [dict() for _ in GROUP_BITS]
    for (g, mask), value in mine.items():
        packed[g][mask] = swap(value, mask) if mask else value
    tokens, mine = lax.optimization_barrier((tokens, mine))
    hidden, saved_acts = forward(tokens, w_up, w_down)
    near = exchange_hidden(hidden)
    up_terms, down_terms = backward(saved_acts, d_logits, w_up, w_down, w_out)
    terms = [(proj_up[l], *up_terms[l]) for l in range(layers)] + [(proj_down[l], *down_terms[l]) for l in range(layers)]
    low = project_gradients(terms, DEVICES, me)
    _, _, rank, cols = low.shape
    near, low = lax.optimization_barrier((near, low))
    chunks = len(ROW_CHUNKS)
    results = []
    gathered = []
    for chunk in range(chunks):
        if results:
            near, results[-1][0] = lax.optimization_barrier((near, results[-1][0]))
        results.append(list(reduce_head(near, packed, w_out, mom_out.T, var_out.T, chunk, low)))
        low = results[-1][3] if chunk == 0 else None
        payload = results[-1][0]
        if chunk == 1:
            low_scattered = results[1][3][:, 0]
            m_up, v_up, dir_up = adam_update(low_scattered[:layers], mom_up, var_up)
            m_down, v_down, dir_down = adam_update(low_scattered[layers:].transpose(0, 2, 1), mom_down, var_down)
            dirs = jnp.concatenate([dir_up, dir_down.transpose(0, 2, 1)], axis=0).astype(jnp.bfloat16)
            side = payload.shape[1] // cols
            dirs = dirs.reshape(side, -1, cols).transpose(1, 0, 2).reshape(-1, payload.shape[1])
            payload = jnp.concatenate([payload, dirs], axis=0)
        gathered.append(lax.all_gather(payload, DATA_AXIS, axis=0))
    w_out_new = None
    gathered[0], results[-1][1] = lax.optimization_barrier((gathered[0], results[-1][1]))
    for chunk in range(chunks):
        w_out_new = place_parts(gathered[chunk], vocab, total_rows, chunk, w_out_new)
    dirs = gathered[1][:, ROW_CHUNKS[1]:].reshape(DEVICES, -1, side, cols).transpose(0, 2, 1, 3).reshape(DEVICES, 2 * layers, rank, cols)
    w_up_new, w_down_new = back_project(dirs, w_up, w_down, proj_up, proj_down)
    m_out = jnp.concatenate([r[1] for r in results], axis=1).T
    v_out = jnp.concatenate([r[2] for r in results], axis=1).T
    return w_up_new, w_down_new, w_out_new, m_up, v_up, m_down, v_down, m_out, v_out


def solution(mesh):
    row_spec = P(DATA_AXIS, None)
    whole = P()
    up_spec = P(None, None, DATA_AXIS)
    down_spec = P(None, DATA_AXIS, None)
    head_spec = P(None, DATA_AXIS)
    in_specs = (row_spec, row_spec, whole, whole, whole, whole, whole, up_spec, up_spec, down_spec, down_spec, head_spec, head_spec)
    out_specs = (whole, whole, whole, up_spec, up_spec, down_spec, down_spec, head_spec, head_spec)

    return jax.shard_map(local_step, mesh=mesh, in_specs=in_specs, out_specs=out_specs, check_vma=False)
```

```python
import jax
import jax.numpy as jnp
from jax import lax
from jax.experimental import pallas as pl
from jax.experimental.pallas import tpu as pltpu
from jax.sharding import PartitionSpec as P


BETA1 = 0.9
BETA2 = 0.999
EPS = 1e-8
STEP = 4
LR = 0.02
ALPHA = 0.5
LR_HEAD = 0.01
DATA_AXIS = 'data'
DEVICES = 16
LANES = 128
CORE, X, Y, Z = 1, 2, 4, 8
GROUP_BITS = ((Z, Y, X), (Y, X, Z), (X, Z, Y))
GROUP_TILES = (6, 5, 5)
TERM_BITS = ((X, Y, Z), (Y, Z, X), (Z, X, Y), (Z, Y, X))
LOW_STEPS = (1, 3)
PLACE_SPLIT = 1
TAIL_ROWS = 64
PACKS = (((0, 2),), ((1, 2), (2, 2)), ((0, 3), (1, 3), (2, 3)), ((0, 1), (1, 1), (2, 1)), ((0, 0), (1, 0), (2, 0)))
ROW_CHUNKS = (256, 256, 256)


def gelu_tanh(values):
    return jax.nn.gelu(values, approximate=True)


def adam_update(gradient, moment_one, moment_two):
    moment_one = BETA1 * moment_one + (1.0 - BETA1) * gradient
    moment_two = BETA2 * moment_two + (1.0 - BETA2) * gradient * gradient
    direction = (moment_one * (1.0 / (1.0 - BETA1 ** STEP))) / (jnp.sqrt(moment_two * (1.0 / (1.0 - BETA2 ** STEP))) + EPS)
    return moment_one, moment_two, direction


def swap(values, mask):
    return lax.ppermute(values, DATA_AXIS, [(i, i ^ mask) for i in range(DEVICES)])


def partner_mask(group, partner):
    bit = GROUP_BITS[group][0]
    return (0, CORE, bit, bit | CORE)[partner]


def group_offsets():
    offsets = [0]
    for tiles in GROUP_TILES:
        offsets.append(offsets[-1] + tiles * LANES)
    return offsets


def shift_left(ref, rows, first, tiles, shift, lane):
    last = ref.shape[1] // LANES - 1

    def rolled(index):
        at = pl.multiple_of(jnp.minimum(first + index, last) * LANES, LANES)
        return pltpu.roll(ref[rows, pl.ds(at, LANES)], (LANES - shift) % LANES, 1)

    pieces = []
    left = rolled(0)
    for index in range(tiles):
        right = rolled(index + 1)
        pieces.append(jnp.where(lane < LANES - shift, left, right))
        left = right
    return pieces


def pack_columns(values, jobs, shard_cols):
    rows, total = values.shape
    count = jobs[0][0].shape[0]
    row_block = 256
    tables, in_specs, out_specs, out_shapes = [], [], [], []
    for j, (owners, offset, width) in enumerate(jobs):
        window = width + LANES
        starts = owners * shard_cols + offset
        tiles = starts // LANES
        bases = jnp.minimum(tiles, (total - window) // LANES)
        tables.append(jnp.stack([bases, tiles - bases, starts % LANES]))
        in_specs.append(pl.BlockSpec((pl.Element(rows), pl.Element(window)), lambda s, t, j=j: (0, pl.multiple_of(t[j, 0, s] * LANES, LANES))))
        out_specs.append(pl.BlockSpec((1, rows, width), lambda s, t: (s, 0, 0)))
        out_shapes.append(jax.ShapeDtypeStruct((count, rows, width), jnp.bfloat16))

    def body(table_ref, *refs):
        entry = pl.program_id(0)

        def selector(depth, cols, by):
            source = lax.broadcasted_iota(jnp.int32, (depth, cols), 0)
            target = lax.broadcasted_iota(jnp.int32, (depth, cols), 1)
            return jnp.where(source == target + by, 1.0, 0.0).astype(jnp.bfloat16)

        plans = []
        for j, (_, _, width) in enumerate(jobs):
            first, shift = table_ref[j, 1, entry], table_ref[j, 2, entry]
            tail = width % (2 * LANES) or 2 * LANES
            by_roll = len(jobs) > 2 and j == len(jobs) - 1
            selectors = None if by_roll else (selector(3 * LANES, 2 * LANES, shift), selector(tail + LANES, tail, shift + first * LANES))
            plans.append((refs[j], refs[len(jobs) + j], width, tail, first, shift, selectors))
        lane = lax.broadcasted_iota(jnp.int32, (row_block, LANES), 1)

        def step(i, carry):
            sl = pl.ds(pl.multiple_of(i * row_block, row_block), row_block)
            for in_ref, out_ref, width, tail, first, shift, selectors in plans:
                if selectors is None:
                    for t, piece in enumerate(shift_left(in_ref, sl, first, width // LANES, shift, lane)):
                        out_ref[0, sl, t * LANES:(t + 1) * LANES] = piece
                    continue
                inner, outer = selectors
                for at in range(0, width - tail, 2 * LANES):
                    source = in_ref[sl, pl.ds(pl.multiple_of(first * LANES + at, LANES), 3 * LANES)]
                    out_ref[0, sl, at:at + 2 * LANES] = jnp.dot(source, inner, preferred_element_type=jnp.float32).astype(jnp.bfloat16)
                at = width - tail
                out_ref[0, sl, at:] = jnp.dot(in_ref[sl, at:], outer, preferred_element_type=jnp.float32).astype(jnp.bfloat16)
            return carry

        lax.fori_loop(0, rows // row_block, step, 0)

    moved = sum(count * rows * width for _, _, width in jobs)
    return pl.pallas_call(
        body,
        grid_spec=pltpu.PrefetchScalarGridSpec(num_scalar_prefetch=1, grid=(count,), in_specs=in_specs, out_specs=out_specs),
        out_shape=out_shapes,
        cost_estimate=pl.CostEstimate(flops=moved * 768, bytes_accessed=moved * 4, transcendentals=0),
        name='pack_columns',
    )(jnp.stack(tables), *[values] * len(jobs))


def project_gradients(terms, owners, me):
    count = len(terms)
    model, rank = terms[0][0].shape
    tokens, hidden = terms[0][2].shape
    cols = hidden // owners
    step_owners = 8
    block = step_owners * cols

    rel = jnp.arange(owners, dtype=jnp.int32) ^ me
    table = jnp.stack([sum(jnp.where(rel & bit, owners >> (k + 1), 0) for k, bit in enumerate((CORE, *bits))) for bits in TERM_BITS])

    def body(table_ref, *refs):
        out_ref, turned, left, right, middle = refs[-5:]
        term = pl.program_id(0)
        for m in range(count):
            p_ref, h_ref, e_ref = refs[3 * m:3 * m + 3]

            @pl.when(term == m)
            def _():
                @pl.when(pl.program_id(1) == 0)
                def _():
                    left[...] = p_ref[...]
                    right[...] = h_ref[...]

                def move(i, carry):
                    sl = pl.ds(pl.multiple_of(i * 64, 64), 64)
                    middle[sl] = e_ref[sl]
                    return carry

                lax.fori_loop(0, tokens // 64, move, 0)

        @pl.when(pl.program_id(1) == 0)
        def _():
            turned[...] = right[...].T

        gradient = jnp.dot(turned[...], middle[...], preferred_element_type=jnp.float32)
        high = gradient.astype(jnp.bfloat16)
        low = (gradient - high.astype(jnp.float32)).astype(jnp.bfloat16)
        total = jnp.dot(left[...], high, preferred_element_type=jnp.float32) + jnp.dot(left[...], low, preferred_element_type=jnp.float32)
        for k in range(step_owners):
            out_ref[0, table_ref[term, pl.program_id(1) * step_owners + k]] = total[:, k * cols:(k + 1) * cols]

    in_specs, operands = [], []
    for m, (p, h, e) in enumerate(terms):
        in_specs += [pl.BlockSpec((rank, model), lambda t, c, _: (0, 0)), pl.BlockSpec((tokens, model), lambda t, c, _: (0, 0)),
                     pl.BlockSpec((tokens, block), lambda t, c, _, m=m: (0, jnp.where(t == m, c, jnp.where(t < m, 0, hidden // block - 1))))]
        operands += [p.T, h, e]
    return pl.pallas_call(
        body,
        grid_spec=pltpu.PrefetchScalarGridSpec(
            num_scalar_prefetch=1,
            grid=(count, hidden // block),
            in_specs=in_specs,
            out_specs=pl.BlockSpec((1, owners, rank, cols), lambda t, c, _: (t, 0, 0, 0)),
            scratch_shapes=[pltpu.VMEM(dims, jnp.bfloat16) for dims in ((model, tokens), (rank, model), (tokens, model), (tokens, block))],
        ),
        out_shape=jax.ShapeDtypeStruct((count, owners, rank, cols), jnp.float32),
        cost_estimate=pl.CostEstimate(flops=count * 2 * model * hidden * (tokens + 2 * rank), bytes_accessed=count * hidden * (tokens * 2 + rank * 4), transcendentals=0),
        name='project_gradients',
    )(table, *operands)


def reduce_head(near, packed, w_out, mom_out, var_out, chunk, low=None):
    groups = len(GROUP_BITS)
    offsets = group_offsets()
    row_chunk = ROW_CHUNKS[chunk]
    places = 0 if low is None else low.shape[1]
    low_steps = 0 if low is None else LOW_STEPS[chunk]
    low_done = sum(LOW_STEPS[:chunk])
    last_tile = (w_out.shape[1] - offsets[-1] - LANES) // LANES
    shard_cols = mom_out.shape[0]
    owners, tokens, _ = packed[0][0].shape
    widths = [offsets[g + 1] - offsets[g] for g in range(groups)]
    masks = [(0, CORE, bit, bit | CORE) for bit, _, _ in GROUP_BITS]
    near_keys = sorted(near)

    def body(*refs):
        near_refs = dict(zip(near_keys, refs))
        refs = refs[len(near_keys):]
        if low is not None:
            low_ref, refs = refs[0], refs[1:]
        packed_refs = [refs[4 * g:4 * g + 4] for g in range(groups)]
        refs = refs[4 * groups:]
        w_ref, mom_ref, var_ref, w_out_ref, mom_out_ref, var_out_ref = refs[:6]
        refs = refs[6:]
        if low is not None:
            low_out_ref, low_buf, *low_got, low_load, low_send, low_recv = refs[:5 + low_steps]
            refs = refs[5 + low_steps:]
        near_buf, near_sem, w_window, *refs = refs
        blocks, refs = refs[:groups], refs[groups:]
        part, refs = refs[:groups], refs[groups:]
        got, refs = refs[:groups], refs[groups:]
        got_own, refs = refs[:groups], refs[groups:]
        w_buf, mom_buf, var_buf, mom_turned, var_turned, load_sem, first_send, first_recv, second_send, second_recv, state_sem = refs
        me = lax.axis_index(DATA_AXIS)
        barrier = pltpu.get_barrier_semaphore()
        greeted = (X, Y, Z, CORE) if low is not None and chunk == 0 else (X, Y, Z)
        for bit in greeted:
            pl.semaphore_signal(barrier, inc=1, device_id=(me ^ bit,), device_id_type=pl.DeviceIdType.MESH)

        def load(g, entry):
            return [pltpu.make_async_copy(packed_refs[g][k].at[entry], blocks[g].at[k], load_sem.at[g, k]) for k in range(4)]

        for g in range(groups):
            for copy in load(g, 3):
                copy.start()
        rows = pl.ds(sum(ROW_CHUNKS[:chunk]), row_chunk)
        valid = pl.ds(0, shard_cols)
        own_tile = (me * shard_cols) // LANES
        base_tile = jnp.minimum(own_tile, last_tile)
        window = pl.ds(pl.multiple_of(base_tile * LANES, LANES), offsets[-1] + LANES)
        state = [pltpu.make_async_copy(w_ref.at[rows, window], w_window, state_sem.at[0]),
                 pltpu.make_async_copy(mom_ref.at[:, rows], mom_turned.at[valid], state_sem.at[1]),
                 pltpu.make_async_copy(var_ref.at[:, rows], var_turned.at[valid], state_sem.at[2])]
        near_loads = [pltpu.make_async_copy(near_refs[masks[g][k]].at[rows], near_buf.at[g, k], near_sem.at[g, k]) for g in range(groups) for k in range(4)]
        for copy in near_loads:
            copy.start()
        for copy in state:
            copy.start()
        pl.semaphore_wait(barrier, len(greeted))

        def low_copy(at, term):
            half = places >> (at + 1)
            source = low_ref if at == 0 else low_buf
            return pltpu.make_async_remote_copy(
                src_ref=source.at[term, pl.ds(half, half)], dst_ref=low_got[at].at[term], send_sem=low_send.at[at, term], recv_sem=low_recv.at[at, term],
                device_id=(me ^ (CORE, *TERM_BITS[term])[low_done + at],), device_id_type=pl.DeviceIdType.MESH)

        def low_step(at):
            half = places >> (at + 1)
            for term in range(len(TERM_BITS)):
                low_copy(at, term).wait_recv()

                def add(e, carry):
                    low_buf[term, e] = low_buf[term, e] + low_got[at][term, e]
                    return carry

                lax.fori_loop(0, half, add, 0)
                if at + 1 < low_steps:
                    low_copy(at + 1, term).start()

        if low is not None:
            keep = pl.ds(0, places // 2)
            low_loads = [pltpu.make_async_copy(low_ref.at[term, keep], low_buf.at[term], low_load.at[term]) for term in range(len(TERM_BITS))]
            for term, copy in enumerate(low_loads):
                low_copy(0, term).start()
                copy.start()
        for copy in near_loads:
            copy.wait()

        def first_copy(g, entry):
            return pltpu.make_async_remote_copy(
                src_ref=part[g].at[entry], dst_ref=got[g].at[entry - 2], send_sem=first_send.at[g, entry - 2], recv_sem=first_recv.at[g, entry - 2],
                device_id=(me ^ GROUP_BITS[g][1],), device_id_type=pl.DeviceIdType.MESH)

        def second_copy(g):
            return pltpu.make_async_remote_copy(
                src_ref=part[g].at[1], dst_ref=got_own[g], send_sem=second_send.at[g], recv_sem=second_recv.at[g],
                device_id=(me ^ GROUP_BITS[g][2],), device_id_type=pl.DeviceIdType.MESH)

        def step(i, carry):
            entry = 3 - i
            for g in range(groups):
                for copy in load(g, entry):
                    copy.wait()

                def accumulate(k, carry):
                    term = jnp.dot(near_buf[g, k], blocks[g][k], preferred_element_type=jnp.float32)

                    @pl.when(k == 0)
                    def _():
                        part[g][entry] = term

                    @pl.when(k > 0)
                    def _():
                        part[g][entry] = part[g][entry] + term

                    return carry

                lax.fori_loop(0, 4, accumulate, 0)

                @pl.when(i < 3)
                def _():
                    for copy in load(g, entry - 1):
                        copy.start()

                @pl.when(i == 0)
                def _():
                    first_copy(g, 3).start()

                @pl.when(i == 1)
                def _():
                    first_copy(g, 2).start()

                @pl.when(i == 2)
                def _():
                    first_copy(g, 3).wait_recv()
                    part[g][1] = part[g][1] + got[g][1]
                    second_copy(g).start()
            return carry

        lax.fori_loop(0, 4, step, 0)

        if low is not None:
            for copy in low_loads:
                copy.wait()
            low_step(0)
        for copy in state:
            copy.wait()
        lane = lax.broadcasted_iota(jnp.int32, (64, LANES), 1)

        def align(i, carry):
            sl = pl.ds(pl.multiple_of(i * 64, 64), 64)
            for t, piece in enumerate(shift_left(w_window, sl, own_tile - base_tile, offsets[-1] // LANES, (me * shard_cols) % LANES, lane)):
                w_buf[sl, t * LANES:(t + 1) * LANES] = piece
            return carry

        lax.fori_loop(0, row_chunk // 64, align, 0)

        def turn_in(i, carry):
            for k in range(2):
                cols = pl.ds(pl.multiple_of((2 * i + k) * LANES, LANES), LANES)
                mom_buf[:, cols] = mom_turned[cols].T
                var_buf[:, cols] = var_turned[cols].T
            return carry

        lax.fori_loop(0, offsets[-1] // (2 * LANES), turn_in, 0)
        block = 32
        for g in range(groups):
            first_copy(g, 2).wait_recv()
        if low_steps > 1:
            low_step(1)
        for g in range(groups):
            second_copy(g).wait_recv()
            cols = slice(offsets[g], offsets[g + 1])

            def adam(i, carry):
                sl = pl.ds(pl.multiple_of(i * block, block), block)
                gradient = part[g][0, sl] + got[g][0, sl] + got_own[g][sl]
                m_new, v_new, direction = adam_update(gradient, mom_buf[sl, cols], var_buf[sl, cols])
                mom_buf[sl, cols] = m_new
                var_buf[sl, cols] = v_new
                w_buf[sl, cols] = (w_buf[sl, cols].astype(jnp.float32) - LR_HEAD * direction).astype(jnp.bfloat16)
                return carry

            lax.fori_loop(0, row_chunk // block, adam, 0)
        results = [pltpu.make_async_copy(w_buf, w_out_ref, state_sem.at[0]),
                   pltpu.make_async_copy(mom_turned.at[valid], mom_out_ref, state_sem.at[1]),
                   pltpu.make_async_copy(var_turned.at[valid], var_out_ref, state_sem.at[2])]
        results[0].start()

        def turn_out(i, carry):
            for k in range(4):
                cols = pl.ds(pl.multiple_of((4 * i + k) * LANES, LANES), LANES)
                mom_turned[cols] = mom_buf[:, cols].T
                var_turned[cols] = var_buf[:, cols].T
            return carry

        lax.fori_loop(0, offsets[-1] // (4 * LANES), turn_out, 0)
        results[1].start()
        results[2].start()
        if low is not None:
            if low_steps > 2:
                low_step(2)
            results += [pltpu.make_async_copy(low_buf.at[term, pl.ds(0, places >> low_steps)], low_out_ref.at[term], low_load.at[term]) for term in range(len(TERM_BITS))]
            for copy in results[3:]:
                copy.start()
            for at in range(low_steps):
                for term in range(len(TERM_BITS)):
                    low_copy(at, term).wait_send()
        for g in range(groups):
            first_copy(g, 3).wait_send()
            first_copy(g, 2).wait_send()
            second_copy(g).wait_send()
        for copy in results:
            copy.wait()

    anywhere = pl.BlockSpec(memory_space=pl.ANY)
    out_shapes = [jax.ShapeDtypeStruct((row_chunk, offsets[-1]), jnp.bfloat16)] + [jax.ShapeDtypeStruct((shard_cols, row_chunk), jnp.float32)] * 2
    scratch = []
    if low is not None:
        terms, _, rank, cols = low.shape
        out_shapes.append(jax.ShapeDtypeStruct((terms, places >> low_steps, rank, cols), jnp.float32))
        scratch.append(pltpu.VMEM((terms, places // 2, rank, cols), jnp.float32))
        scratch += [pltpu.VMEM((terms, places >> (at + 1), rank, cols), jnp.float32) for at in range(low_steps)]
        scratch += [pltpu.SemaphoreType.DMA((terms,)), pltpu.SemaphoreType.DMA((low_steps, terms)), pltpu.SemaphoreType.DMA((low_steps, terms))]
    scratch += [pltpu.VMEM((groups, 4, row_chunk, tokens), jnp.bfloat16), pltpu.SemaphoreType.DMA((groups, 4)), pltpu.VMEM((row_chunk, offsets[-1] + LANES), jnp.bfloat16)]
    scratch += [pltpu.VMEM((4, tokens, w), jnp.bfloat16) for w in widths]
    scratch += [pltpu.VMEM((owners, row_chunk, w), jnp.float32) for w in widths]
    scratch += [pltpu.VMEM((2, row_chunk, w), jnp.float32) for w in widths]
    scratch += [pltpu.VMEM((row_chunk, w), jnp.float32) for w in widths]
    scratch += [pltpu.VMEM((row_chunk, offsets[-1]), jnp.bfloat16)]
    scratch += [pltpu.VMEM((row_chunk, offsets[-1]), jnp.float32)] * 2 + [pltpu.VMEM((offsets[-1], row_chunk), jnp.float32)] * 2
    scratch += [pltpu.SemaphoreType.DMA((groups, 4)), pltpu.SemaphoreType.DMA((groups, 2)), pltpu.SemaphoreType.DMA((groups, 2)),
                pltpu.SemaphoreType.DMA((groups,)), pltpu.SemaphoreType.DMA((groups,)), pltpu.SemaphoreType.DMA((3,))]
    return pl.pallas_call(
        body,
        in_specs=[anywhere] * (len(near_keys) + 4 * groups + 3 + (low is not None)),
        out_specs=[anywhere] * len(out_shapes),
        out_shape=out_shapes,
        scratch_shapes=scratch,
        cost_estimate=pl.CostEstimate(flops=60_000_000_000, bytes_accessed=100_000_000, transcendentals=0),
        compiler_params=pltpu.CompilerParams(collective_id=chunk, has_side_effects=True, vmem_limit_bytes=60 * 1024 * 1024),
        name='reduce_head',
    )(*[near[k] for k in near_keys], *([] if low is None else [low]), *[packed[g][m] for g in range(groups) for m in masks[g]], w_out, mom_out, var_out)


def gather_rows(values, first_row):
    total, width = values.shape
    count = total - first_row
    groups = len(GROUP_BITS)
    offsets = group_offsets()
    hops = []
    for bit, first, second in GROUP_BITS:
        known = [0]
        moves = []
        for axis in (bit, first, second, CORE):
            moves += [(rel, axis) for rel in known]
            known += [rel | axis for rel in known]
        hops.append(moves)

    def body(values_ref, out_ref, own_sem, send_sem, recv_sem):
        me = lax.axis_index(DATA_AXIS)
        barrier = pltpu.get_barrier_semaphore()
        for bit in (X, Y, Z, CORE):
            pl.semaphore_signal(barrier, inc=1, device_id=(me ^ bit,), device_id_type=pl.DeviceIdType.MESH)
        own = pltpu.make_async_copy(values_ref.at[pl.ds(first_row, count)], out_ref.at[me], own_sem)
        own.start()
        pl.semaphore_wait(barrier, 4)
        own.wait()

        def hop(g, rel, axis):
            at = hops[g].index((rel, axis))
            block = out_ref.at[me ^ rel, :, pl.ds(offsets[g], offsets[g + 1] - offsets[g])]
            return pltpu.make_async_remote_copy(
                src_ref=block, dst_ref=block, send_sem=send_sem.at[g, at], recv_sem=recv_sem.at[g, at],
                device_id=(me ^ axis,), device_id_type=pl.DeviceIdType.MESH)

        def arrival(g, rel, axis):
            at = hops[g].index((rel, axis))
            block = out_ref.at[me ^ rel ^ axis, :, pl.ds(offsets[g], offsets[g + 1] - offsets[g])]
            return pltpu.make_async_remote_copy(
                src_ref=block, dst_ref=block, send_sem=send_sem.at[g, at], recv_sem=recv_sem.at[g, at],
                device_id=(me ^ axis,), device_id_type=pl.DeviceIdType.MESH)

        for g in range(groups):
            for axis in (*GROUP_BITS[g], CORE):
                hop(g, 0, axis).start()
        for step in range(7):
            for g in range(groups):
                bit, first, second = GROUP_BITS[g]
                rel, axis = ((0, bit), (0, first), (bit, first), (0, second), (bit, second), (first, second), (bit | first, second))[step]
                arrival(g, rel, axis).wait_recv()
                later = {bit: (first, second, CORE), first: (second, CORE), second: (CORE,)}[axis]
                for onward in later:
                    hop(g, rel | axis, onward).start()
        for g in range(groups):
            for rel, axis in hops[g]:
                if axis == CORE:
                    arrival(g, rel, axis).wait_recv()
        for g in range(groups):
            for rel, axis in hops[g]:
                hop(g, rel, axis).wait_send()

    return pl.pallas_call(
        body,
        in_specs=[pl.BlockSpec(memory_space=pl.ANY)],
        out_specs=pl.BlockSpec(memory_space=pltpu.VMEM),
        out_shape=jax.ShapeDtypeStruct((DEVICES, count, width), values.dtype),
        scratch_shapes=[pltpu.SemaphoreType.DMA, pltpu.SemaphoreType.DMA((groups, 15)), pltpu.SemaphoreType.DMA((groups, 15))],
        cost_estimate=pl.CostEstimate(flops=10_000_000_000, bytes_accessed=10_000_000, transcendentals=0),
        compiler_params=pltpu.CompilerParams(collective_id=len(ROW_CHUNKS), has_side_effects=True),
        name='gather_rows',
    )(values)


def place_parts(parts, vocab, total_rows, start_row, count_rows, previous):
    shard_cols = vocab // DEVICES
    rows = 32
    count = -(-shard_cols // LANES)
    share = DEVICES // PLACE_SPLIT

    def body(*refs):
        part_refs, out_ref = refs[:PLACE_SPLIT], refs[-1]
        lane = lax.broadcasted_iota(jnp.int32, (rows, LANES), 1)
        pending = None
        for owner in range(DEVICES):
            base, shift = divmod(owner * shard_cols, LANES)
            rolled = []
            for index in range(count):
                piece = part_refs[owner // share][owner % share, :, index * LANES:(index + 1) * LANES]
                rolled.append(pltpu.roll(piece, shift, 1) if shift else piece)
            end = owner * shard_cols + shard_cols
            for tile in range(base, -(-end // LANES)):
                index = tile - base
                if shift == 0:
                    value = rolled[index]
                elif index == 0:
                    value = jnp.where(lane < shift, pending, rolled[0])
                elif index == count:
                    value = rolled[count - 1]
                else:
                    value = jnp.where(lane < shift, rolled[index - 1], rolled[index])
                if (tile + 1) * LANES <= end:
                    out_ref[:, tile * LANES:(tile + 1) * LANES] = value
                else:
                    pending = value

    steps = count_rows // rows
    start = start_row // rows
    in_specs = [pl.BlockSpec((share, rows, count * LANES), lambda s, k=k: (k, s, 0)) for k in range(PLACE_SPLIT)]
    operands = [parts] * PLACE_SPLIT
    aliases = {}
    if previous is not None:
        in_specs.append(pl.BlockSpec(memory_space=pl.ANY))
        operands.append(previous)
        aliases = {PLACE_SPLIT: 0}
    return pl.pallas_call(
        body,
        grid=(steps,),
        in_specs=in_specs,
        out_specs=pl.BlockSpec((rows, vocab), lambda s: (start + s, 0)),
        out_shape=jax.ShapeDtypeStruct((total_rows, vocab), jnp.bfloat16),
        input_output_aliases=aliases,
        cost_estimate=pl.CostEstimate(flops=count_rows * vocab * 16, bytes_accessed=count_rows * vocab * 4, transcendentals=0),
        name='place_parts',
    )(*operands)


def back_project(gathered, w_up, w_down, proj_up, proj_down):
    layers, model, hidden = w_up.shape
    _, _, rank, cols = gathered.shape
    step_owners = 4
    block = step_owners * cols

    def body(up_dir_ref, down_dir_ref, w_up_ref, w_down_ref, p_ref, q_ref, up_ref, down_ref):
        up_dir = jnp.concatenate([up_dir_ref[k, 0] for k in range(step_owners)], axis=1)
        down_dir = jnp.concatenate([down_dir_ref[k, 0] for k in range(step_owners)], axis=1)
        step_up = jnp.dot(p_ref[0], up_dir, preferred_element_type=jnp.float32)
        up_ref[0] = (w_up_ref[0].astype(jnp.float32) - LR * ALPHA * step_up).astype(jnp.bfloat16)
        step_down = lax.dot_general(down_dir, q_ref[0], (((0,), (1,)), ((), ())), preferred_element_type=jnp.float32)
        down_ref[0] = (w_down_ref[0].astype(jnp.float32) - LR * ALPHA * step_down).astype(jnp.bfloat16)

    up_spec = pl.BlockSpec((1, model, block), lambda l, c: (l, 0, c))
    down_spec = pl.BlockSpec((1, block, model), lambda l, c: (l, c, 0))
    proj_spec = pl.BlockSpec((1, model, rank), lambda l, c: (l, 0, 0))
    return pl.pallas_call(
        body,
        grid=(layers, hidden // block),
        in_specs=[pl.BlockSpec((step_owners, 1, rank, cols), lambda l, c: (c, l, 0, 0)),
                  pl.BlockSpec((step_owners, 1, rank, cols), lambda l, c: (c, layers + l, 0, 0)),
                  up_spec, down_spec, proj_spec, proj_spec],
        out_specs=[up_spec, down_spec],
        out_shape=[jax.ShapeDtypeStruct(w_up.shape, jnp.bfloat16), jax.ShapeDtypeStruct(w_down.shape, jnp.bfloat16)],
        cost_estimate=pl.CostEstimate(flops=8 * model * hidden * rank, bytes_accessed=30_000_000, transcendentals=0),
        name='back_project',
    )(gathered, gathered, w_up, w_down, proj_up, proj_down)


def forward(tokens, w_up, w_down):
    num_layers = w_up.shape[0]
    hidden = tokens
    saved_acts = []
    for layer_idx in range(num_layers):
        pre_act = jnp.dot(hidden, w_up[layer_idx], preferred_element_type=jnp.float32).astype(jnp.bfloat16)
        post_act = gelu_tanh(pre_act.astype(jnp.float32)).astype(jnp.bfloat16)
        saved_acts.append((hidden, pre_act, post_act))
        hidden = (hidden.astype(jnp.float32) + jnp.dot(post_act, w_down[layer_idx], preferred_element_type=jnp.float32)).astype(jnp.bfloat16)
    return hidden, saved_acts


def backward(saved_acts, d_logits, w_up, w_down, w_out):
    num_layers = w_up.shape[0]
    grad_hidden = jnp.einsum('tv,dv->td', d_logits, w_out, preferred_element_type=jnp.float32).astype(jnp.bfloat16)
    up_terms = [None] * num_layers
    down_terms = [None] * num_layers
    for layer_idx in reversed(range(num_layers)):
        hidden_in, pre_act, post_act = saved_acts[layer_idx]
        down_terms[layer_idx] = (grad_hidden, post_act)
        d_post = jnp.einsum('td,fd->tf', grad_hidden, w_down[layer_idx], preferred_element_type=jnp.float32)
        gelu_pull = jax.vjp(gelu_tanh, pre_act.astype(jnp.float32))[1]
        d_pre = gelu_pull(d_post)[0].astype(jnp.bfloat16)
        up_terms[layer_idx] = (hidden_in, d_pre)
        if layer_idx > 0:
            grad_hidden = (grad_hidden.astype(jnp.float32) + jnp.einsum('tf,df->td', d_pre, w_up[layer_idx], preferred_element_type=jnp.float32)).astype(jnp.bfloat16)
    return up_terms, down_terms


def exchange_hidden(hidden):
    near = {0: hidden.T}
    near[CORE] = swap(near[0], CORE)
    for bit in (Z, Y, X):
        near[bit] = swap(near[0], bit)
    for bit in (Z, Y, X):
        near[bit | CORE] = swap(near[bit], CORE)
    return near


def local_step(tokens, d_logits, w_up, w_down, w_out, proj_up, proj_down, mom_up, var_up, mom_down, var_down, mom_out, var_out):
    me = lax.axis_index(DATA_AXIS)
    layers = w_up.shape[0]
    total_rows, vocab = w_out.shape
    shard_cols = mom_out.shape[1]
    offsets = group_offsets()
    mine = {}
    for pack in PACKS:
        jobs, keys = [], []
        for g, partner in pack:
            _, first, second = GROUP_BITS[g]
            mask = partner_mask(g, partner)
            rels = jnp.array([0, second, first, first | second], jnp.int32) ^ mask
            jobs.append((rels ^ me, offsets[g], offsets[g + 1] - offsets[g]))
            keys.append((g, mask))
        for key, value in zip(keys, pack_columns(d_logits, jobs, shard_cols)):
            mine[key] = value
    packed = [dict() for _ in GROUP_BITS]
    for (g, mask), value in mine.items():
        packed[g][mask] = swap(value, mask) if mask else value
    tokens, mine = lax.optimization_barrier((tokens, mine))
    hidden, saved_acts = forward(tokens, w_up, w_down)
    near = exchange_hidden(hidden)
    up_terms, down_terms = backward(saved_acts, d_logits, w_up, w_down, w_out)
    terms = [(proj_up[l], *up_terms[l]) for l in range(layers)] + [(proj_down[l], *down_terms[l]) for l in range(layers)]
    low = project_gradients(terms, DEVICES, me)
    _, _, rank, cols = low.shape
    near, low = lax.optimization_barrier((near, low))
    chunks = len(ROW_CHUNKS)
    results = []
    gathered = []
    for chunk in range(chunks):
        if results:
            near, results[-1][0] = lax.optimization_barrier((near, results[-1][0]))
        results.append(list(reduce_head(near, packed, w_out, mom_out.T, var_out.T, chunk, low)))
        low = results[-1][3] if chunk == 0 else None
        payload = results[-1][0]
        if chunk == chunks - 1:
            payload = payload[:-TAIL_ROWS]
        if chunk == 1:
            low_scattered = results[1][3][:, 0]
            m_up, v_up, dir_up = adam_update(low_scattered[:layers], mom_up, var_up)
            m_down, v_down, dir_down = adam_update(low_scattered[layers:].transpose(0, 2, 1), mom_down, var_down)
            dirs = jnp.concatenate([dir_up, dir_down.transpose(0, 2, 1)], axis=0).astype(jnp.bfloat16)
            side = payload.shape[1] // cols
            dirs = dirs.reshape(side, -1, cols).transpose(1, 0, 2).reshape(-1, payload.shape[1])
            payload = jnp.concatenate([payload, dirs], axis=0)
        gathered.append(lax.all_gather(payload, DATA_AXIS, axis=0))
    w_out_new = None
    gathered.append(gather_rows(results[-1][0], ROW_CHUNKS[-1] - TAIL_ROWS))
    gathered[0], gathered[-1] = lax.optimization_barrier((gathered[0], gathered[-1]))
    pieces = list(zip(gathered[:-2], ROW_CHUNKS)) + [(gathered[-1], TAIL_ROWS), (gathered[-2], ROW_CHUNKS[-1] - TAIL_ROWS)]
    starts = [sum(ROW_CHUNKS[:k]) for k in range(chunks - 1)] + [total_rows - TAIL_ROWS, total_rows - ROW_CHUNKS[-1]]
    for (piece, count), start in zip(pieces, starts):
        w_out_new = place_parts(piece, vocab, total_rows, start, count, w_out_new)
    dirs = gathered[1][:, ROW_CHUNKS[1]:].reshape(DEVICES, -1, side, cols).transpose(0, 2, 1, 3).reshape(DEVICES, 2 * layers, rank, cols)
    w_up_new, w_down_new = back_project(dirs, w_up, w_down, proj_up, proj_down)
    m_out = jnp.concatenate([r[1] for r in results], axis=1).T
    v_out = jnp.concatenate([r[2] for r in results], axis=1).T
    return w_up_new, w_down_new, w_out_new, m_up, v_up, m_down, v_down, m_out, v_out


def solution(mesh):
    row_spec = P(DATA_AXIS, None)
    whole = P()
    up_spec = P(None, None, DATA_AXIS)
    down_spec = P(None, DATA_AXIS, None)
    head_spec = P(None, DATA_AXIS)
    in_specs = (row_spec, row_spec, whole, whole, whole, whole, whole, up_spec, up_spec, down_spec, down_spec, head_spec, head_spec)
    out_specs = (whole, whole, whole, up_spec, up_spec, down_spec, down_spec, head_spec, head_spec)

    return jax.shard_map(local_step, mesh=mesh, in_specs=in_specs, out_specs=out_specs, check_vma=False)
```

```python
import jax
import jax.numpy as jnp
from jax import lax
from jax.experimental import pallas as pl
from jax.experimental.pallas import tpu as pltpu
from jax.sharding import PartitionSpec as P


BETA1 = 0.9
BETA2 = 0.999
EPS = 1e-8
STEP = 4
LR = 0.02
ALPHA = 0.5
LR_HEAD = 0.01
DATA_AXIS = 'data'
DEVICES = 16
LANES = 128
CORE, X, Y, Z = 1, 2, 4, 8
GROUP_BITS = ((Z, Y, X), (Y, X, Z), (X, Z, Y))
GROUP_TILES = (6, 5, 5)
TERM_BITS = ((X, Y, Z), (Y, Z, X), (Z, X, Y), (Z, Y, X))
LOW_STEPS = (1, 3)
PLACE_SPLIT = 1
TAIL_ROWS = 96
PACKS = (((0, 2),), ((1, 2), (2, 2)), ((0, 3), (1, 3), (2, 3)), ((0, 1), (1, 1), (2, 1)), ((0, 0), (1, 0), (2, 0)))
ROW_CHUNKS = (256, 256, 256)


def gelu_tanh(values):
    return jax.nn.gelu(values, approximate=True)


def adam_update(gradient, moment_one, moment_two):
    moment_one = BETA1 * moment_one + (1.0 - BETA1) * gradient
    moment_two = BETA2 * moment_two + (1.0 - BETA2) * gradient * gradient
    direction = (moment_one * (1.0 / (1.0 - BETA1 ** STEP))) / (jnp.sqrt(moment_two * (1.0 / (1.0 - BETA2 ** STEP))) + EPS)
    return moment_one, moment_two, direction


def swap(values, mask):
    return lax.ppermute(values, DATA_AXIS, [(i, i ^ mask) for i in range(DEVICES)])


def partner_mask(group, partner):
    bit = GROUP_BITS[group][0]
    return (0, CORE, bit, bit | CORE)[partner]


def group_offsets():
    offsets = [0]
    for tiles in GROUP_TILES:
        offsets.append(offsets[-1] + tiles * LANES)
    return offsets


def shift_left(ref, rows, first, tiles, shift, lane):
    last = ref.shape[1] // LANES - 1

    def rolled(index):
        at = pl.multiple_of(jnp.minimum(first + index, last) * LANES, LANES)
        return pltpu.roll(ref[rows, pl.ds(at, LANES)], (LANES - shift) % LANES, 1)

    pieces = []
    left = rolled(0)
    for index in range(tiles):
        right = rolled(index + 1)
        pieces.append(jnp.where(lane < LANES - shift, left, right))
        left = right
    return pieces


def pack_columns(values, jobs, shard_cols):
    rows, total = values.shape
    count = jobs[0][0].shape[0]
    row_block = 256
    tables, in_specs, out_specs, out_shapes = [], [], [], []
    for j, (owners, offset, width) in enumerate(jobs):
        window = width + LANES
        starts = owners * shard_cols + offset
        tiles = starts // LANES
        bases = jnp.minimum(tiles, (total - window) // LANES)
        tables.append(jnp.stack([bases, tiles - bases, starts % LANES]))
        in_specs.append(pl.BlockSpec((pl.Element(rows), pl.Element(window)), lambda s, t, j=j: (0, pl.multiple_of(t[j, 0, s] * LANES, LANES))))
        out_specs.append(pl.BlockSpec((1, rows, width), lambda s, t: (s, 0, 0)))
        out_shapes.append(jax.ShapeDtypeStruct((count, rows, width), jnp.bfloat16))

    def body(table_ref, *refs):
        entry = pl.program_id(0)

        def selector(depth, cols, by):
            source = lax.broadcasted_iota(jnp.int32, (depth, cols), 0)
            target = lax.broadcasted_iota(jnp.int32, (depth, cols), 1)
            return jnp.where(source == target + by, 1.0, 0.0).astype(jnp.bfloat16)

        plans = []
        for j, (_, _, width) in enumerate(jobs):
            first, shift = table_ref[j, 1, entry], table_ref[j, 2, entry]
            tail = width % (2 * LANES) or 2 * LANES
            by_roll = len(jobs) > 2 and j == len(jobs) - 1
            selectors = None if by_roll else (selector(3 * LANES, 2 * LANES, shift), selector(tail + LANES, tail, shift + first * LANES))
            plans.append((refs[j], refs[len(jobs) + j], width, tail, first, shift, selectors))
        lane = lax.broadcasted_iota(jnp.int32, (row_block, LANES), 1)

        def step(i, carry):
            sl = pl.ds(pl.multiple_of(i * row_block, row_block), row_block)
            for in_ref, out_ref, width, tail, first, shift, selectors in plans:
                if selectors is None:
                    for t, piece in enumerate(shift_left(in_ref, sl, first, width // LANES, shift, lane)):
                        out_ref[0, sl, t * LANES:(t + 1) * LANES] = piece
                    continue
                inner, outer = selectors
                for at in range(0, width - tail, 2 * LANES):
                    source = in_ref[sl, pl.ds(pl.multiple_of(first * LANES + at, LANES), 3 * LANES)]
                    out_ref[0, sl, at:at + 2 * LANES] = jnp.dot(source, inner, preferred_element_type=jnp.float32).astype(jnp.bfloat16)
                at = width - tail
                out_ref[0, sl, at:] = jnp.dot(in_ref[sl, at:], outer, preferred_element_type=jnp.float32).astype(jnp.bfloat16)
            return carry

        lax.fori_loop(0, rows // row_block, step, 0)

    moved = sum(count * rows * width for _, _, width in jobs)
    return pl.pallas_call(
        body,
        grid_spec=pltpu.PrefetchScalarGridSpec(num_scalar_prefetch=1, grid=(count,), in_specs=in_specs, out_specs=out_specs),
        out_shape=out_shapes,
        cost_estimate=pl.CostEstimate(flops=moved * 768, bytes_accessed=moved * 4, transcendentals=0),
        name='pack_columns',
    )(jnp.stack(tables), *[values] * len(jobs))


def project_gradients(terms, owners, me):
    count = len(terms)
    model, rank = terms[0][0].shape
    tokens, hidden = terms[0][2].shape
    cols = hidden // owners
    step_owners = 8
    block = step_owners * cols

    rel = jnp.arange(owners, dtype=jnp.int32) ^ me
    table = jnp.stack([sum(jnp.where(rel & bit, owners >> (k + 1), 0) for k, bit in enumerate((CORE, *bits))) for bits in TERM_BITS])

    def body(table_ref, *refs):
        out_ref, turned, left, right, middle = refs[-5:]
        term = pl.program_id(0)
        for m in range(count):
            p_ref, h_ref, e_ref = refs[3 * m:3 * m + 3]

            @pl.when(term == m)
            def _():
                @pl.when(pl.program_id(1) == 0)
                def _():
                    left[...] = p_ref[...]
                    right[...] = h_ref[...]

                def move(i, carry):
                    sl = pl.ds(pl.multiple_of(i * 64, 64), 64)
                    middle[sl] = e_ref[sl]
                    return carry

                lax.fori_loop(0, tokens // 64, move, 0)

        @pl.when(pl.program_id(1) == 0)
        def _():
            turned[...] = right[...].T

        gradient = jnp.dot(turned[...], middle[...], preferred_element_type=jnp.float32)
        high = gradient.astype(jnp.bfloat16)
        low = (gradient - high.astype(jnp.float32)).astype(jnp.bfloat16)
        total = jnp.dot(left[...], high, preferred_element_type=jnp.float32) + jnp.dot(left[...], low, preferred_element_type=jnp.float32)
        for k in range(step_owners):
            out_ref[0, table_ref[term, pl.program_id(1) * step_owners + k]] = total[:, k * cols:(k + 1) * cols]

    in_specs, operands = [], []
    for m, (p, h, e) in enumerate(terms):
        in_specs += [pl.BlockSpec((rank, model), lambda t, c, _: (0, 0)), pl.BlockSpec((tokens, model), lambda t, c, _: (0, 0)),
                     pl.BlockSpec((tokens, block), lambda t, c, _, m=m: (0, jnp.where(t == m, c, jnp.where(t < m, 0, hidden // block - 1))))]
        operands += [p.T, h, e]
    return pl.pallas_call(
        body,
        grid_spec=pltpu.PrefetchScalarGridSpec(
            num_scalar_prefetch=1,
            grid=(count, hidden // block),
            in_specs=in_specs,
            out_specs=pl.BlockSpec((1, owners, rank, cols), lambda t, c, _: (t, 0, 0, 0)),
            scratch_shapes=[pltpu.VMEM(dims, jnp.bfloat16) for dims in ((model, tokens), (rank, model), (tokens, model), (tokens, block))],
        ),
        out_shape=jax.ShapeDtypeStruct((count, owners, rank, cols), jnp.float32),
        cost_estimate=pl.CostEstimate(flops=count * 2 * model * hidden * (tokens + 2 * rank), bytes_accessed=count * hidden * (tokens * 2 + rank * 4), transcendentals=0),
        name='project_gradients',
    )(table, *operands)


def reduce_head(near, packed, w_out, mom_out, var_out, chunk, low=None):
    groups = len(GROUP_BITS)
    offsets = group_offsets()
    row_chunk = ROW_CHUNKS[chunk]
    places = 0 if low is None else low.shape[1]
    low_steps = 0 if low is None else LOW_STEPS[chunk]
    low_done = sum(LOW_STEPS[:chunk])
    last_tile = (w_out.shape[1] - offsets[-1] - LANES) // LANES
    shard_cols = mom_out.shape[0]
    owners, tokens, _ = packed[0][0].shape
    widths = [offsets[g + 1] - offsets[g] for g in range(groups)]
    masks = [(0, CORE, bit, bit | CORE) for bit, _, _ in GROUP_BITS]
    near_keys = sorted(near)

    def body(*refs):
        near_refs = dict(zip(near_keys, refs))
        refs = refs[len(near_keys):]
        if low is not None:
            low_ref, refs = refs[0], refs[1:]
        packed_refs = [refs[4 * g:4 * g + 4] for g in range(groups)]
        refs = refs[4 * groups:]
        w_ref, mom_ref, var_ref, w_out_ref, mom_out_ref, var_out_ref = refs[:6]
        refs = refs[6:]
        if low is not None:
            low_out_ref, low_buf, *low_got, low_load, low_send, low_recv = refs[:5 + low_steps]
            refs = refs[5 + low_steps:]
        near_buf, near_sem, w_window, *refs = refs
        blocks, refs = refs[:groups], refs[groups:]
        part, refs = refs[:groups], refs[groups:]
        got, refs = refs[:groups], refs[groups:]
        got_own, refs = refs[:groups], refs[groups:]
        w_buf, mom_buf, var_buf, mom_turned, var_turned, load_sem, first_send, first_recv, second_send, second_recv, state_sem = refs
        me = lax.axis_index(DATA_AXIS)
        barrier = pltpu.get_barrier_semaphore()
        greeted = (X, Y, Z, CORE) if low is not None and chunk == 0 else (X, Y, Z)
        for bit in greeted:
            pl.semaphore_signal(barrier, inc=1, device_id=(me ^ bit,), device_id_type=pl.DeviceIdType.MESH)

        def load(g, entry):
            return [pltpu.make_async_copy(packed_refs[g][k].at[entry], blocks[g].at[k], load_sem.at[g, k]) for k in range(4)]

        for g in range(groups):
            for copy in load(g, 3):
                copy.start()
        rows = pl.ds(sum(ROW_CHUNKS[:chunk]), row_chunk)
        valid = pl.ds(0, shard_cols)
        own_tile = (me * shard_cols) // LANES
        base_tile = jnp.minimum(own_tile, last_tile)
        window = pl.ds(pl.multiple_of(base_tile * LANES, LANES), offsets[-1] + LANES)
        state = [pltpu.make_async_copy(w_ref.at[rows, window], w_window, state_sem.at[0]),
                 pltpu.make_async_copy(mom_ref.at[:, rows], mom_turned.at[valid], state_sem.at[1]),
                 pltpu.make_async_copy(var_ref.at[:, rows], var_turned.at[valid], state_sem.at[2])]
        near_loads = [pltpu.make_async_copy(near_refs[masks[g][k]].at[rows], near_buf.at[g, k], near_sem.at[g, k]) for g in range(groups) for k in range(4)]
        for copy in near_loads:
            copy.start()
        for copy in state:
            copy.start()
        pl.semaphore_wait(barrier, len(greeted))

        def low_copy(at, term):
            half = places >> (at + 1)
            source = low_ref if at == 0 else low_buf
            return pltpu.make_async_remote_copy(
                src_ref=source.at[term, pl.ds(half, half)], dst_ref=low_got[at].at[term], send_sem=low_send.at[at, term], recv_sem=low_recv.at[at, term],
                device_id=(me ^ (CORE, *TERM_BITS[term])[low_done + at],), device_id_type=pl.DeviceIdType.MESH)

        def low_step(at):
            half = places >> (at + 1)
            for term in range(len(TERM_BITS)):
                low_copy(at, term).wait_recv()

                def add(e, carry):
                    low_buf[term, e] = low_buf[term, e] + low_got[at][term, e]
                    return carry

                lax.fori_loop(0, half, add, 0)
                if at + 1 < low_steps:
                    low_copy(at + 1, term).start()

        if low is not None:
            keep = pl.ds(0, places // 2)
            low_loads = [pltpu.make_async_copy(low_ref.at[term, keep], low_buf.at[term], low_load.at[term]) for term in range(len(TERM_BITS))]
            for term, copy in enumerate(low_loads):
                low_copy(0, term).start()
                copy.start()
        for copy in near_loads:
            copy.wait()

        def first_copy(g, entry):
            return pltpu.make_async_remote_copy(
                src_ref=part[g].at[entry], dst_ref=got[g].at[entry - 2], send_sem=first_send.at[g, entry - 2], recv_sem=first_recv.at[g, entry - 2],
                device_id=(me ^ GROUP_BITS[g][1],), device_id_type=pl.DeviceIdType.MESH)

        def second_copy(g):
            return pltpu.make_async_remote_copy(
                src_ref=part[g].at[1], dst_ref=got_own[g], send_sem=second_send.at[g], recv_sem=second_recv.at[g],
                device_id=(me ^ GROUP_BITS[g][2],), device_id_type=pl.DeviceIdType.MESH)

        def step(i, carry):
            entry = 3 - i
            for g in range(groups):
                for copy in load(g, entry):
                    copy.wait()

                def accumulate(k, carry):
                    term = jnp.dot(near_buf[g, k], blocks[g][k], preferred_element_type=jnp.float32)

                    @pl.when(k == 0)
                    def _():
                        part[g][entry] = term

                    @pl.when(k > 0)
                    def _():
                        part[g][entry] = part[g][entry] + term

                    return carry

                lax.fori_loop(0, 4, accumulate, 0)

                @pl.when(i < 3)
                def _():
                    for copy in load(g, entry - 1):
                        copy.start()

                @pl.when(i == 0)
                def _():
                    first_copy(g, 3).start()

                @pl.when(i == 1)
                def _():
                    first_copy(g, 2).start()

                @pl.when(i == 2)
                def _():
                    first_copy(g, 3).wait_recv()
                    part[g][1] = part[g][1] + got[g][1]
                    second_copy(g).start()
            return carry

        lax.fori_loop(0, 4, step, 0)

        if low is not None:
            for copy in low_loads:
                copy.wait()
            low_step(0)
        for copy in state:
            copy.wait()
        lane = lax.broadcasted_iota(jnp.int32, (64, LANES), 1)

        def align(i, carry):
            sl = pl.ds(pl.multiple_of(i * 64, 64), 64)
            for t, piece in enumerate(shift_left(w_window, sl, own_tile - base_tile, offsets[-1] // LANES, (me * shard_cols) % LANES, lane)):
                w_buf[sl, t * LANES:(t + 1) * LANES] = piece
            return carry

        lax.fori_loop(0, row_chunk // 64, align, 0)

        def turn_in(i, carry):
            for k in range(2):
                cols = pl.ds(pl.multiple_of((2 * i + k) * LANES, LANES), LANES)
                mom_buf[:, cols] = mom_turned[cols].T
                var_buf[:, cols] = var_turned[cols].T
            return carry

        lax.fori_loop(0, offsets[-1] // (2 * LANES), turn_in, 0)
        block = 32
        for g in range(groups):
            first_copy(g, 2).wait_recv()
        if low_steps > 1:
            low_step(1)
        for g in range(groups):
            second_copy(g).wait_recv()
            cols = slice(offsets[g], offsets[g + 1])

            def adam(i, carry):
                sl = pl.ds(pl.multiple_of(i * block, block), block)
                gradient = part[g][0, sl] + got[g][0, sl] + got_own[g][sl]
                m_new, v_new, direction = adam_update(gradient, mom_buf[sl, cols], var_buf[sl, cols])
                mom_buf[sl, cols] = m_new
                var_buf[sl, cols] = v_new
                w_buf[sl, cols] = (w_buf[sl, cols].astype(jnp.float32) - LR_HEAD * direction).astype(jnp.bfloat16)
                return carry

            lax.fori_loop(0, row_chunk // block, adam, 0)
        results = [pltpu.make_async_copy(w_buf, w_out_ref, state_sem.at[0]),
                   pltpu.make_async_copy(mom_turned.at[valid], mom_out_ref, state_sem.at[1]),
                   pltpu.make_async_copy(var_turned.at[valid], var_out_ref, state_sem.at[2])]
        results[0].start()

        def turn_out(i, carry):
            for k in range(4):
                cols = pl.ds(pl.multiple_of((4 * i + k) * LANES, LANES), LANES)
                mom_turned[cols] = mom_buf[:, cols].T
                var_turned[cols] = var_buf[:, cols].T
            return carry

        lax.fori_loop(0, offsets[-1] // (4 * LANES), turn_out, 0)
        results[1].start()
        results[2].start()
        if low is not None:
            if low_steps > 2:
                low_step(2)
            results += [pltpu.make_async_copy(low_buf.at[term, pl.ds(0, places >> low_steps)], low_out_ref.at[term], low_load.at[term]) for term in range(len(TERM_BITS))]
            for copy in results[3:]:
                copy.start()
            for at in range(low_steps):
                for term in range(len(TERM_BITS)):
                    low_copy(at, term).wait_send()
        for g in range(groups):
            first_copy(g, 3).wait_send()
            first_copy(g, 2).wait_send()
            second_copy(g).wait_send()
        for copy in results:
            copy.wait()

    anywhere = pl.BlockSpec(memory_space=pl.ANY)
    out_shapes = [jax.ShapeDtypeStruct((row_chunk, offsets[-1]), jnp.bfloat16)] + [jax.ShapeDtypeStruct((shard_cols, row_chunk), jnp.float32)] * 2
    scratch = []
    if low is not None:
        terms, _, rank, cols = low.shape
        out_shapes.append(jax.ShapeDtypeStruct((terms, places >> low_steps, rank, cols), jnp.float32))
        scratch.append(pltpu.VMEM((terms, places // 2, rank, cols), jnp.float32))
        scratch += [pltpu.VMEM((terms, places >> (at + 1), rank, cols), jnp.float32) for at in range(low_steps)]
        scratch += [pltpu.SemaphoreType.DMA((terms,)), pltpu.SemaphoreType.DMA((low_steps, terms)), pltpu.SemaphoreType.DMA((low_steps, terms))]
    scratch += [pltpu.VMEM((groups, 4, row_chunk, tokens), jnp.bfloat16), pltpu.SemaphoreType.DMA((groups, 4)), pltpu.VMEM((row_chunk, offsets[-1] + LANES), jnp.bfloat16)]
    scratch += [pltpu.VMEM((4, tokens, w), jnp.bfloat16) for w in widths]
    scratch += [pltpu.VMEM((owners, row_chunk, w), jnp.float32) for w in widths]
    scratch += [pltpu.VMEM((2, row_chunk, w), jnp.float32) for w in widths]
    scratch += [pltpu.VMEM((row_chunk, w), jnp.float32) for w in widths]
    scratch += [pltpu.VMEM((row_chunk, offsets[-1]), jnp.bfloat16)]
    scratch += [pltpu.VMEM((row_chunk, offsets[-1]), jnp.float32)] * 2 + [pltpu.VMEM((offsets[-1], row_chunk), jnp.float32)] * 2
    scratch += [pltpu.SemaphoreType.DMA((groups, 4)), pltpu.SemaphoreType.DMA((groups, 2)), pltpu.SemaphoreType.DMA((groups, 2)),
                pltpu.SemaphoreType.DMA((groups,)), pltpu.SemaphoreType.DMA((groups,)), pltpu.SemaphoreType.DMA((3,))]
    return pl.pallas_call(
        body,
        in_specs=[anywhere] * (len(near_keys) + 4 * groups + 3 + (low is not None)),
        out_specs=[anywhere] * len(out_shapes),
        out_shape=out_shapes,
        scratch_shapes=scratch,
        cost_estimate=pl.CostEstimate(flops=60_000_000_000, bytes_accessed=100_000_000, transcendentals=0),
        compiler_params=pltpu.CompilerParams(collective_id=chunk, has_side_effects=True, vmem_limit_bytes=60 * 1024 * 1024),
        name='reduce_head',
    )(*[near[k] for k in near_keys], *([] if low is None else [low]), *[packed[g][m] for g in range(groups) for m in masks[g]], w_out, mom_out, var_out)


def gather_rows(values, first_row):
    total, width = values.shape
    count = total - first_row
    groups = len(GROUP_BITS)
    offsets = group_offsets()
    hops = []
    for bit, first, second in GROUP_BITS:
        known = [0]
        moves = []
        for axis in (bit, first, second, CORE):
            moves += [(rel, axis) for rel in known]
            known += [rel | axis for rel in known]
        hops.append(moves)

    def body(values_ref, out_ref, own_sem, send_sem, recv_sem):
        me = lax.axis_index(DATA_AXIS)
        barrier = pltpu.get_barrier_semaphore()
        for bit in (X, Y, Z, CORE):
            pl.semaphore_signal(barrier, inc=1, device_id=(me ^ bit,), device_id_type=pl.DeviceIdType.MESH)
        own = pltpu.make_async_copy(values_ref.at[pl.ds(first_row, count)], out_ref.at[me], own_sem)
        own.start()
        pl.semaphore_wait(barrier, 4)
        own.wait()

        def hop(g, rel, axis):
            at = hops[g].index((rel, axis))
            block = out_ref.at[me ^ rel, :, pl.ds(offsets[g], offsets[g + 1] - offsets[g])]
            return pltpu.make_async_remote_copy(
                src_ref=block, dst_ref=block, send_sem=send_sem.at[g, at], recv_sem=recv_sem.at[g, at],
                device_id=(me ^ axis,), device_id_type=pl.DeviceIdType.MESH)

        def arrival(g, rel, axis):
            at = hops[g].index((rel, axis))
            block = out_ref.at[me ^ rel ^ axis, :, pl.ds(offsets[g], offsets[g + 1] - offsets[g])]
            return pltpu.make_async_remote_copy(
                src_ref=block, dst_ref=block, send_sem=send_sem.at[g, at], recv_sem=recv_sem.at[g, at],
                device_id=(me ^ axis,), device_id_type=pl.DeviceIdType.MESH)

        for g in range(groups):
            for axis in (*GROUP_BITS[g], CORE):
                hop(g, 0, axis).start()
        for step in range(7):
            for g in range(groups):
                bit, first, second = GROUP_BITS[g]
                rel, axis = ((0, bit), (0, first), (bit, first), (0, second), (bit, second), (first, second), (bit | first, second))[step]
                arrival(g, rel, axis).wait_recv()
                later = {bit: (first, second, CORE), first: (second, CORE), second: (CORE,)}[axis]
                for onward in later:
                    hop(g, rel | axis, onward).start()
        for g in range(groups):
            for rel, axis in hops[g]:
                if axis == CORE:
                    arrival(g, rel, axis).wait_recv()
        for g in range(groups):
            for rel, axis in hops[g]:
                hop(g, rel, axis).wait_send()

    return pl.pallas_call(
        body,
        in_specs=[pl.BlockSpec(memory_space=pl.ANY)],
        out_specs=pl.BlockSpec(memory_space=pltpu.VMEM),
        out_shape=jax.ShapeDtypeStruct((DEVICES, count, width), values.dtype),
        scratch_shapes=[pltpu.SemaphoreType.DMA, pltpu.SemaphoreType.DMA((groups, 15)), pltpu.SemaphoreType.DMA((groups, 15))],
        cost_estimate=pl.CostEstimate(flops=10_000_000_000, bytes_accessed=10_000_000, transcendentals=0),
        compiler_params=pltpu.CompilerParams(collective_id=len(ROW_CHUNKS), has_side_effects=True),
        name='gather_rows',
    )(values)


def place_parts(parts, vocab, total_rows, start_row, count_rows, previous):
    shard_cols = vocab // DEVICES
    rows = 32
    count = -(-shard_cols // LANES)
    share = DEVICES // PLACE_SPLIT

    def body(*refs):
        part_refs, out_ref = refs[:PLACE_SPLIT], refs[-1]
        lane = lax.broadcasted_iota(jnp.int32, (rows, LANES), 1)
        pending = None
        for owner in range(DEVICES):
            base, shift = divmod(owner * shard_cols, LANES)
            rolled = []
            for index in range(count):
                piece = part_refs[owner // share][owner % share, :, index * LANES:(index + 1) * LANES]
                rolled.append(pltpu.roll(piece, shift, 1) if shift else piece)
            end = owner * shard_cols + shard_cols
            for tile in range(base, -(-end // LANES)):
                index = tile - base
                if shift == 0:
                    value = rolled[index]
                elif index == 0:
                    value = jnp.where(lane < shift, pending, rolled[0])
                elif index == count:
                    value = rolled[count - 1]
                else:
                    value = jnp.where(lane < shift, rolled[index - 1], rolled[index])
                if (tile + 1) * LANES <= end:
                    out_ref[:, tile * LANES:(tile + 1) * LANES] = value
                else:
                    pending = value

    steps = count_rows // rows
    start = start_row // rows
    in_specs = [pl.BlockSpec((share, rows, count * LANES), lambda s, k=k: (k, s, 0)) for k in range(PLACE_SPLIT)]
    operands = [parts] * PLACE_SPLIT
    aliases = {}
    if previous is not None:
        in_specs.append(pl.BlockSpec(memory_space=pl.ANY))
        operands.append(previous)
        aliases = {PLACE_SPLIT: 0}
    return pl.pallas_call(
        body,
        grid=(steps,),
        in_specs=in_specs,
        out_specs=pl.BlockSpec((rows, vocab), lambda s: (start + s, 0)),
        out_shape=jax.ShapeDtypeStruct((total_rows, vocab), jnp.bfloat16),
        input_output_aliases=aliases,
        cost_estimate=pl.CostEstimate(flops=count_rows * vocab * 16, bytes_accessed=count_rows * vocab * 4, transcendentals=0),
        name='place_parts',
    )(*operands)


def back_project(gathered, first_row, w_up, w_down, proj_up, proj_down):
    layers, model, hidden = w_up.shape
    owners, _, width = gathered.shape
    rank, cols = proj_up.shape[2], hidden // owners
    depth = 2 * layers * rank * cols // width
    step_owners = 4
    block = step_owners * cols

    def direction(ref, term):
        parts = []
        for k in range(step_owners):
            lanes = [pl.ds(pl.multiple_of((term * (rank // depth) + q) * cols, cols), cols) for q in range(rank // depth)]
            parts.append(jnp.concatenate([ref[k, :, at] for at in lanes], axis=0))
        return jnp.concatenate(parts, axis=1)

    def body(dir_ref, w_up_ref, w_down_ref, p_ref, q_ref, up_ref, down_ref):
        layer = pl.program_id(0)
        up_dir = direction(dir_ref, layer)
        down_dir = direction(dir_ref, layers + layer)
        step_up = jnp.dot(p_ref[0], up_dir, preferred_element_type=jnp.float32)
        up_ref[0] = (w_up_ref[0].astype(jnp.float32) - LR * ALPHA * step_up).astype(jnp.bfloat16)
        step_down = lax.dot_general(down_dir, q_ref[0], (((0,), (1,)), ((), ())), preferred_element_type=jnp.float32)
        down_ref[0] = (w_down_ref[0].astype(jnp.float32) - LR * ALPHA * step_down).astype(jnp.bfloat16)

    up_spec = pl.BlockSpec((1, model, block), lambda l, c: (l, 0, c))
    down_spec = pl.BlockSpec((1, block, model), lambda l, c: (l, c, 0))
    proj_spec = pl.BlockSpec((1, model, rank), lambda l, c: (l, 0, 0))
    return pl.pallas_call(
        body,
        grid=(layers, hidden // block),
        in_specs=[pl.BlockSpec((step_owners, depth, width), lambda l, c: (c, first_row // depth, 0)),
                  up_spec, down_spec, proj_spec, proj_spec],
        out_specs=[up_spec, down_spec],
        out_shape=[jax.ShapeDtypeStruct(w_up.shape, jnp.bfloat16), jax.ShapeDtypeStruct(w_down.shape, jnp.bfloat16)],
        cost_estimate=pl.CostEstimate(flops=8 * model * hidden * rank, bytes_accessed=30_000_000, transcendentals=0),
        name='back_project',
    )(gathered, w_up, w_down, proj_up, proj_down)


def forward(tokens, w_up, w_down):
    layers, model, hidden = w_up.shape
    rows = tokens.shape[0]
    block = 512
    row_block = 256
    blocks = hidden // block

    def body(tokens_ref, w_up_ref, w_down_ref, *refs):
        pre_refs, post_refs = refs[:layers], refs[layers:2 * layers]
        state_refs, turned_ref, state, total = refs[2 * layers:-3], refs[-3], refs[-2], refs[-1]
        layer, step = pl.program_id(0), pl.program_id(1)

        @pl.when(jnp.logical_and(layer == 0, step == 0))
        def _():
            state[...] = tokens_ref[...]

        @pl.when(step == 0)
        def _():
            total[...] = jnp.zeros_like(total)

        def part(i, carry):
            sl = pl.ds(pl.multiple_of(i * row_block, row_block), row_block)
            pre = jnp.dot(state[sl], w_up_ref[0], preferred_element_type=jnp.float32).astype(jnp.bfloat16)
            post = gelu_tanh(pre.astype(jnp.float32)).astype(jnp.bfloat16)
            for m in range(layers):
                @pl.when(layer == m)
                def _():
                    pre_refs[m][sl] = pre
                    post_refs[m][sl] = post
            total[sl] += jnp.dot(post, w_down_ref[0], preferred_element_type=jnp.float32)
            return carry

        lax.fori_loop(0, rows // row_block, part, 0)

        @pl.when(step == blocks - 1)
        def _():
            def finish(i, carry):
                sl = pl.ds(pl.multiple_of(i * 128, 128), 128)
                new = (state[sl].astype(jnp.float32) + total[sl]).astype(jnp.bfloat16)
                state[sl] = new
                for m in range(layers - 1):
                    @pl.when(layer == m)
                    def _():
                        state_refs[m][sl] = new
                turned_ref[:, sl] = new.T
                return carry

            lax.fori_loop(0, rows // 128, finish, 0)

    act_specs = [pl.BlockSpec((rows, block), lambda l, c, m=m: (0, jnp.where(l == m, c, jnp.where(l < m, 0, blocks - 1)))) for m in range(layers)]
    act_shapes = [jax.ShapeDtypeStruct((rows, hidden), jnp.bfloat16)] * layers
    state_specs = [pl.BlockSpec((rows, model), lambda l, c: (0, 0))] * (layers - 1)
    state_shapes = [jax.ShapeDtypeStruct((rows, model), jnp.bfloat16)] * (layers - 1)
    outs = pl.pallas_call(
        body,
        grid=(layers, blocks),
        in_specs=[pl.BlockSpec((rows, model), lambda l, c: (0, 0)),
                  pl.BlockSpec((1, model, block), lambda l, c: (l, 0, c)),
                  pl.BlockSpec((1, block, model), lambda l, c: (l, c, 0))],
        out_specs=[*act_specs, *act_specs, *state_specs, pl.BlockSpec((model, rows), lambda l, c: (0, 0))],
        out_shape=[*act_shapes, *act_shapes, *state_shapes, jax.ShapeDtypeStruct((model, rows), jnp.bfloat16)],
        scratch_shapes=[pltpu.VMEM((rows, model), jnp.bfloat16), pltpu.VMEM((rows, model), jnp.float32)],
        cost_estimate=pl.CostEstimate(flops=4 * layers * rows * model * hidden, bytes_accessed=20_000_000, transcendentals=0),
        name='forward_blocks',
    )(tokens, w_up, w_down)
    states = [tokens, *outs[2 * layers:-1]]
    saved = [(states[m], outs[m], outs[layers + m]) for m in range(layers)]
    return outs[-1], saved


def backward(saved_acts, d_logits, w_up, w_down, w_out):
    num_layers = w_up.shape[0]
    grad_hidden = jnp.einsum('tv,dv->td', d_logits, w_out, preferred_element_type=jnp.float32).astype(jnp.bfloat16)
    up_terms = [None] * num_layers
    down_terms = [None] * num_layers
    for layer_idx in reversed(range(num_layers)):
        hidden_in, pre_act, post_act = saved_acts[layer_idx]
        down_terms[layer_idx] = (grad_hidden, post_act)
        d_post = jnp.einsum('td,fd->tf', grad_hidden, w_down[layer_idx], preferred_element_type=jnp.float32)
        gelu_pull = jax.vjp(gelu_tanh, pre_act.astype(jnp.float32))[1]
        d_pre = gelu_pull(d_post)[0].astype(jnp.bfloat16)
        up_terms[layer_idx] = (hidden_in, d_pre)
        if layer_idx > 0:
            grad_hidden = (grad_hidden.astype(jnp.float32) + jnp.einsum('tf,df->td', d_pre, w_up[layer_idx], preferred_element_type=jnp.float32)).astype(jnp.bfloat16)
    return up_terms, down_terms


def exchange_hidden(hidden_t):
    near = {0: hidden_t}
    near[CORE] = swap(near[0], CORE)
    for bit in (Z, Y, X):
        near[bit] = swap(near[0], bit)
    for bit in (Z, Y, X):
        near[bit | CORE] = swap(near[bit], CORE)
    return near


def local_step(tokens, d_logits, w_up, w_down, w_out, proj_up, proj_down, mom_up, var_up, mom_down, var_down, mom_out, var_out):
    me = lax.axis_index(DATA_AXIS)
    layers = w_up.shape[0]
    total_rows, vocab = w_out.shape
    shard_cols = mom_out.shape[1]
    offsets = group_offsets()
    mine = {}
    for pack in PACKS:
        jobs, keys = [], []
        for g, partner in pack:
            _, first, second = GROUP_BITS[g]
            mask = partner_mask(g, partner)
            rels = jnp.array([0, second, first, first | second], jnp.int32) ^ mask
            jobs.append((rels ^ me, offsets[g], offsets[g + 1] - offsets[g]))
            keys.append((g, mask))
        for key, value in zip(keys, pack_columns(d_logits, jobs, shard_cols)):
            mine[key] = value
    packed = [dict() for _ in GROUP_BITS]
    for (g, mask), value in mine.items():
        packed[g][mask] = swap(value, mask) if mask else value
    tokens, mine = lax.optimization_barrier((tokens, mine))
    hidden_t, saved_acts = forward(tokens, w_up, w_down)
    near = exchange_hidden(hidden_t)
    up_terms, down_terms = backward(saved_acts, d_logits, w_up, w_down, w_out)
    terms = [(proj_up[l], *up_terms[l]) for l in range(layers)] + [(proj_down[l], *down_terms[l]) for l in range(layers)]
    low = project_gradients(terms, DEVICES, me)
    _, _, _, cols = low.shape
    near, low = lax.optimization_barrier((near, low))
    chunks = len(ROW_CHUNKS)
    results = []
    gathered = []
    for chunk in range(chunks):
        if results:
            near, results[-1][0] = lax.optimization_barrier((near, results[-1][0]))
        results.append(list(reduce_head(near, packed, w_out, mom_out.T, var_out.T, chunk, low)))
        low = results[-1][3] if chunk == 0 else None
        payload = results[-1][0]
        if chunk == chunks - 1:
            payload = payload[:-TAIL_ROWS]
        if chunk == 1:
            low_scattered = results[1][3][:, 0]
            m_up, v_up, dir_up = adam_update(low_scattered[:layers], mom_up, var_up)
            m_down, v_down, dir_down = adam_update(low_scattered[layers:].transpose(0, 2, 1), mom_down, var_down)
            dirs = jnp.concatenate([dir_up, dir_down.transpose(0, 2, 1)], axis=0).astype(jnp.bfloat16)
            side = payload.shape[1] // cols
            dirs = dirs.reshape(side, -1, cols).transpose(1, 0, 2).reshape(-1, payload.shape[1])
            payload = jnp.concatenate([payload, dirs], axis=0)
        gathered.append(lax.all_gather(payload, DATA_AXIS, axis=0))
    w_out_new = None
    gathered.append(gather_rows(results[-1][0], ROW_CHUNKS[-1] - TAIL_ROWS))
    gathered[0], gathered[-1] = lax.optimization_barrier((gathered[0], gathered[-1]))
    pieces = list(zip(gathered[:-2], ROW_CHUNKS)) + [(gathered[-1], TAIL_ROWS), (gathered[-2], ROW_CHUNKS[-1] - TAIL_ROWS)]
    starts = [sum(ROW_CHUNKS[:k]) for k in range(chunks - 1)] + [total_rows - TAIL_ROWS, total_rows - ROW_CHUNKS[-1]]
    for (piece, count), start in zip(pieces, starts):
        w_out_new = place_parts(piece, vocab, total_rows, start, count, w_out_new)
    w_up_new, w_down_new = back_project(gathered[1], ROW_CHUNKS[1], w_up, w_down, proj_up, proj_down)
    m_out = jnp.concatenate([r[1] for r in results], axis=1).T
    v_out = jnp.concatenate([r[2] for r in results], axis=1).T
    return w_up_new, w_down_new, w_out_new, m_up, v_up, m_down, v_down, m_out, v_out


def solution(mesh):
    row_spec = P(DATA_AXIS, None)
    whole = P()
    up_spec = P(None, None, DATA_AXIS)
    down_spec = P(None, DATA_AXIS, None)
    head_spec = P(None, DATA_AXIS)
    in_specs = (row_spec, row_spec, whole, whole, whole, whole, whole, up_spec, up_spec, down_spec, down_spec, head_spec, head_spec)
    out_specs = (whole, whole, whole, up_spec, up_spec, down_spec, down_spec, head_spec, head_spec)

    return jax.shard_map(local_step, mesh=mesh, in_specs=in_specs, out_specs=out_specs, check_vma=False)
```
